512 devices in a mesh: level: 8 (over y, core), slab: 64 (over x, z).
Axes of the slice: x: 4, y: 4, z: 16, core: 2. Of those that a mesh axis runs over, the one named last changes fastest.
Arguments:
- coef_fine: float32 [24, 512, 2048], P('level', 'slab'), may hold values from 0.2 to 5
- coef_coarse: float32 [24, 512, 2048], P('level', 'slab'), may hold values from 0.2 to 5
- rhs_field: float32 [512, 2048], P('slab'), may hold values from -6 to 6
- level_counts: int32 [8], P('level'), may hold values from 2 to 3, as said below
Outputs:
- solutions: float32 [24, 512, 2048], P('level', 'slab')
- sample_diffs: float32 [24], P('level')
- level_stats: float32 [8, 2], P('level')
- estimate: float32 [2], replicated
The draws below stay inside these ranges and needn't reach their ends.
Inputs may be any that keep to these rules, and one draw needn't show every extreme that they name: `level_counts`: one level has exactly 3 live samples and another exactly 2.
All inputs are finite; a program needn't handle non-finite values.
Results may differ from the reference program's by a relative error of at most 0.0003.
Values sent between devices are 32-bit elements; how exact they have to be, the bound alone decides.
No kernel may reach another device: no remote copies, remote signals or barrier semaphores. Data moves between devices by JAX's collectives and lax.ppermute only.
A program may use at most 128 MiB of HBM per device.

```python
import math
import jax
import jax.numpy as jnp
from jax import lax

NY = 2048
SAMP = 3
LEVELS = 6
NX = 512
NLEV = 8
SAMPLES = 24


def draw_level_counts(key, part):
    key_pos = jax.random.fold_in(key, 11)
    key_val = jax.random.fold_in(key, 12)
    position = jax.random.randint(key_pos, (), 0, NLEV)
    others = jax.random.randint(key_val, (NLEV,), 2, SAMP + 1)
    index = jnp.arange(NLEV)
    following = (position + 1) % NLEV
    counts = jnp.where(index == position, SAMP, others)
    counts = jnp.where(index == following, 2, counts)
    return counts.astype(jnp.int32)


def block_levels(stream_key, extent, cuts, low, top_value):
    def one(axis_at, parts):
        steps = jax.random.uniform(jax.random.fold_in(jax.random.fold_in(stream_key, 6), axis_at), (parts,), jnp.float32, low / len(cuts), top_value / len(cuts))
        return jnp.repeat(jnp.exp(steps), extent[axis_at] // parts).reshape((-1,) + (1,) * (len(extent) - axis_at - 1))

    level = one(*cuts[0])
    for cut in cuts[1:]:
        level = level * one(*cut)
    return level


def noise(stream_key, extent, spread, most, shards=(), kind=jnp.bfloat16):
    entries = jax.random.normal(stream_key, extent, jnp.float32) * spread
    if len(shards) > 0:
        entries = block_levels(stream_key, extent, shards, -0.22, 0.18) * entries
    return jnp.clip(entries, min=-most, max=most).astype(kind)


def setup_inputs(seed: int = 0) -> dict:
    splits = jax.random.split(jax.random.key(seed), 5)
    coef_fine = jnp.clip(jnp.exp(math.log(5.0) - 3.218876 * jax.random.uniform(splits[0], (SAMPLES, NX, NY), jnp.float32) ** block_levels(splits[0], (SAMPLES, NX, NY), ((0, 8), (1, 64)), -0.2, 0.2)), 0.2, 5.0)
    coef_coarse = jnp.clip(jnp.exp(math.log(5.0) - 3.218876 * jax.random.uniform(splits[1], (SAMPLES, NX, NY), jnp.float32) ** block_levels(splits[1], (SAMPLES, NX, NY), ((0, 8), (1, 64)), -0.2, 0.2)), 0.2, 5.0)
    rhs_field = noise(splits[2], (NX, NY), 1.0, 6.0, ((0, 64),), jnp.float32)
    level_counts = draw_level_counts(jax.random.fold_in(splits[4], 71), 0)
    return dict(coef_fine=coef_fine, coef_coarse=coef_coarse, rhs_field=rhs_field, level_counts=level_counts)


OMEGA = 0.8
coarse_sweeps = 4


def pad_all(field):
    return jnp.pad(field, ((0, 0), (1, 1), (1, 1)))


def neighbour_slices():
    return ((slice(None, -2), slice(1, -1)), (slice(2, None), slice(1, -1)), (slice(1, -1), slice(None, -2)), (slice(1, -1), slice(2, None)))


def operator_parts(padded, iterate, conduct_pad, step_scale):
    conduct = conduct_pad[:, 1:-1, 1:-1]
    total = jnp.zeros_like(iterate)
    diagonal = jnp.zeros_like(iterate)
    for rows_cut, cols_cut in neighbour_slices():
        face = 0.5 * (conduct + conduct_pad[:, rows_cut, cols_cut])
        total = total + face * (iterate - padded[:, rows_cut, cols_cut])
        diagonal = diagonal + face
    return step_scale * total, step_scale * diagonal


def coarsen(field):
    batch, rows_here, cols_here = field.shape
    return field.reshape(batch, rows_here // 2, 2, cols_here // 2, 2).mean(axis=(2, 4))


def prolong(field):
    return jnp.repeat(jnp.repeat(field, 2, axis=1), 2, axis=2)


def vcycle(depth, iterate, source, conduct_list):
    step_scale = 0.25 ** depth
    conduct_pad = conduct_list[depth]

    def relax_once(field):
        applied, diagonal = operator_parts(pad_all(field), field, conduct_pad, step_scale)
        return field + OMEGA * (source - applied) / diagonal

    if depth == len(conduct_list) - 1:
        for sweep in range(coarse_sweeps):
            iterate = relax_once(iterate)
        return iterate
    iterate = relax_once(iterate)
    applied, diagonal = operator_parts(pad_all(iterate), iterate, conduct_pad, step_scale)
    coarse_source = coarsen(source - applied)
    correction = vcycle(depth + 1, jnp.zeros_like(coarse_source), coarse_source, conduct_list)
    iterate = iterate + prolong(correction)
    return relax_once(iterate)


def solve_pair(pair, rhs_field):
    conduct = jnp.stack([pair[0], pair[1]])
    source = jnp.broadcast_to(rhs_field, conduct.shape)
    conduct_list = []
    for depth in range(LEVELS):
        conduct_list.append(pad_all(conduct))
        if depth < LEVELS - 1:
            conduct = coarsen(conduct)
    iterate = vcycle(0, jnp.zeros_like(source), source, conduct_list)
    quantity = jnp.sum(iterate, axis=(1, 2)) / (NX * NY)
    return iterate[0], quantity[0] - quantity[1]


def reference(coef_fine, coef_coarse, rhs_field, level_counts):
    solutions, sample_diffs = lax.map(lambda pair: solve_pair(pair, rhs_field), (coef_fine, coef_coarse))
    grouped = sample_diffs.reshape(NLEV, SAMP)
    live = (jnp.arange(SAMP)[None, :] < level_counts[:, None]).astype(jnp.float32)
    counted = level_counts.astype(jnp.float32)
    level_mean = jnp.sum(live * grouped, axis=1) / counted
    level_var = jnp.sum(live * (grouped - level_mean[:, None]) ** 2, axis=1) / jnp.maximum(counted - 1.0, 1.0)
    level_stats = jnp.stack([level_mean, level_var], axis=1)
    estimate = jnp.stack([jnp.sum(level_mean), jnp.sum(level_var / counted)])
    return solutions, sample_diffs, level_stats, estimate
```

```python
import functools

import jax
import jax.numpy as jnp
from jax import lax
from jax.experimental import pallas as pl
from jax.experimental.pallas import tpu as pltpu
from jax.sharding import Mesh
from jax.sharding import PartitionSpec as P

OMEGA = 0.8
SLAB = ("slab_0", "slab_1")
ROWS = 40
F32 = jnp.float32


def iota(shape, dim):
    return lax.broadcasted_iota(jnp.int32, shape, dim)


def right_of(x, cols):
    n = x.shape[1]
    return jnp.where(iota(x.shape, 1) == cols - 1, 0.0, pltpu.roll(x, n - 1, 1))


def below(x, period):
    n = x.shape[0]
    shifted = pltpu.roll(x, n - 1, 0)
    if period is None:
        return shifted
    return jnp.where(iota(x.shape, 0) % period == period - 1, 0.0, shifted)


def faces(k, cols, period):
    half = 0.5 * k
    first = iota(k.shape, 1) == 0
    fr = half + right_of(half, cols)
    fl = jnp.where(first, half, pltpu.roll(fr, 1, 1))
    fd = half + below(half, period)
    fu = pltpu.roll(fd, 1, 0)
    if period is not None:
        fu = jnp.where(iota(k.shape, 0) % period == 0, half, fu)
    return half, fr, fd, (fr + fl) + (fd + fu)


def fluxes(u, half, fr, fd, cols, period):
    q = fr * (u - right_of(u, cols))
    edge = -half * u
    ql = jnp.where(iota(u.shape, 1) == 0, edge, pltpu.roll(q, 1, 1))
    p = fd * (u - below(u, period))
    pu = pltpu.roll(p, 1, 0)
    if period is not None:
        pu = jnp.where(iota(u.shape, 0) % period == 0, edge, pu)
    return (q - ql) + (p - pu)


def pair_matrix(shape, dim, value):
    long, short = iota(shape, dim), iota(shape, 1 - dim)
    return jnp.where(long // 2 == short, value, 0.0).astype(F32)


def dot(a, b):
    return jnp.dot(a, b, precision=lax.Precision.HIGHEST, preferred_element_type=F32)


def pieces(x):
    return [x[:, i : i + 128] for i in range(0, x.shape[1], 128)]


def halve_rows(x, scratch):
    rows = x.shape[0]
    room = -(-rows // 16) * 16
    parts = pieces(x)
    for i, piece in enumerate(parts):
        scratch[i * room : i * room + rows, :] = piece
    out = room // 2
    got = scratch[pl.ds(0, len(parts) * out, stride=2), :] + scratch[pl.ds(1, len(parts) * out, stride=2), :]
    return jnp.concatenate([got[i * out : (i + 1) * out] for i in range(len(parts))], axis=1)


def halve_cols(xs, quarter):
    wide = 256 if xs[0].shape[1] >= 256 else 128
    n = xs[0].shape[1] // wide
    rows = [x.shape[0] for x in xs]
    tall = jnp.concatenate([x[:, i * wide : (i + 1) * wide] for x in xs for i in range(n)], axis=0)
    got = dot(tall, quarter[:wide])
    outs, at = [], 0
    for r in rows:
        outs.append(jnp.concatenate([got[at + i * r : at + (i + 1) * r] for i in range(n)], axis=1))
        at += n * r
    return outs


def double_cols(x, spread):
    n = max(x.shape[1] // 128, 1)
    rows = x.shape[0]
    tall = jnp.concatenate([x[:, i * 128 : (i + 1) * 128] for i in range(n)], axis=0)
    got = dot(tall, spread)
    return jnp.concatenate([got[i * rows : (i + 1) * rows] for i in range(n)], axis=1)


def double_rows(x, scratch, out_rows):
    rows = x.shape[0]
    parts = pieces(x)
    for i, piece in enumerate(parts):
        scratch[pl.ds(i * 2 * rows, rows, stride=2), :] = piece
        scratch[pl.ds(i * 2 * rows + 1, rows, stride=2), :] = piece
    return jnp.concatenate([scratch[i * 2 * rows : i * 2 * rows + out_rows, :] for i in range(len(parts))], axis=1)


def row_mask(shape, depth, edge_ref):
    row = iota(shape, 0)
    return (row >= (edge_ref[0] >> depth)) & (row < (edge_ref[1] >> depth))


def down_kernel(
    edge, kf, kc, g, kfu, kcu, gu, kfd, kcd, gd,
    packed, v0_out, v1_out, v2_out, s1_out, s2_out, k1_out, k2_out, to_below, to_above,
    scratch, parts,
):
    scratch[...] = jnp.zeros_like(scratch)
    quarter = pair_matrix((256, 128), 0, 0.25)
    slots = kf.shape[0]
    ncol = kf.shape[2]
    copies = packed.shape[0]
    source = jnp.concatenate([gu[...], g[...], gd[...]], axis=0)
    for i in range(copies):
        packed[i] = jnp.zeros(packed.shape[1:], F32)
    to_below[...] = jnp.zeros_like(to_below)
    to_above[...] = jnp.zeros_like(to_above)

    def one(slot, fine):
        field = slot if fine else slots + slot
        ku, ko, kd = (kfu, kf, kfd) if fine else (kcu, kc, kcd)
        k = jnp.concatenate([ku[slot], ko[slot], kd[slot]], axis=0)
        s, w = source, jnp.ones_like(source)
        total = jnp.zeros((8, 128), F32)
        for depth in range(3):
            rows, cols = k.shape
            own = 8 >> depth
            half, fr, fd, diag = faces(k, cols, None)
            inside = row_mask(k.shape, depth, edge)
            scale = jnp.where(inside, OMEGA / diag, 0.0)
            us, uw = scale * s, scale * w
            rs = s - fluxes(us, half, fr, fd, cols, None)
            rw = w - fluxes(uw, half, fr, fd, cols, None)
            share = rw * us + uw * s
            if depth == 0:
                share = share[8:16]
            else:
                row = iota(share.shape, 0)
                share = jnp.where((row >= own) & (row < 2 * own), share, 0.0)
            share = functools.reduce(jnp.add, [share[i : i + 8] for i in range(0, share.shape[0], 8)])
            share = functools.reduce(jnp.add, [share[:, i : i + 128] for i in range(0, cols, 128)])
            total = total + share * (16.0**depth)
            if fine:
                v = us * (4.0**depth)
                if depth == 0:
                    v0_out[slot] = v
                if depth == 1:
                    v1_out[slot], s1_out[slot], k1_out[slot] = v, s, k
                if depth == 2:
                    v2_out[slot], s2_out[slot], k2_out[slot] = v, s, k
                    to_below[pl.ds(slot, 1), :] = v[2:3]
                    to_above[pl.ds(slot, 1), :] = v[3:4]
            k, s, w = halve_cols([halve_rows(x, scratch) for x in (k, rs, rw)], quarter)
        for q, x in enumerate((k, s, w)):
            for half_at in range(2):
                line = x[1:2, half_at * 128 : (half_at + 1) * 128]
                for i in range(copies):
                    packed[i, pl.ds((q * 2 * slots + field) * 2 + half_at, 1), :] = line
        parts[pl.ds(field * 8, 8), :] = total

    def body(slot, _):
        one(slot, True)
        one(slot, False)
        return 0

    lax.fori_loop(0, slots, body, 0)
    lane = iota((1, 128), 1)
    line = jnp.zeros((1, 128), F32)
    for field in range(2 * slots):
        line = line + jnp.where(lane == field, jnp.sum(parts[field * 8 : field * 8 + 8]), 0.0)
    for i in range(copies):
        packed[i, 6 * slots * 2 : 6 * slots * 2 + 1, :] = line
    del ncol


def coarse_kernel(place, counts, gathered, e3, stats, message, scratch, whole, *, slots, slabs, cells):
    fields = 2 * slots
    quarter = pair_matrix((256, 128), 0, 0.25)
    spread = pair_matrix((128, 256), 1, 1.0)

    def taken(q):
        halves = [
            jnp.concatenate(
                [gathered[pl.ds((q * fields + f) * 2 + h, slabs, stride=ROWS), :] for f in range(fields)], axis=0
            )
            for h in range(2)
        ]
        return jnp.concatenate(halves, axis=1)

    def halved(xs):
        return halve_cols([halve_rows(x, scratch) for x in xs], quarter)

    k3, s3, w3 = taken(0), taken(1), taken(2)
    n = slabs
    half3, fr3, fd3, diag3 = faces(k3, 256, n)
    scale3 = OMEGA / diag3
    u3 = scale3 * s3
    k4, s4 = halved((k3, s3 - fluxes(u3, half3, fr3, fd3, 256, n)))
    half4, fr4, fd4, diag4 = faces(k4, 128, n // 2)
    scale4 = OMEGA / diag4
    u4 = scale4 * s4
    k5, s5 = halved((k4, s4 - fluxes(u4, half4, fr4, fd4, 128, n // 2)))
    half5, fr5, fd5, diag5 = faces(k5, 64, n // 4)
    scale5 = jnp.where(iota(diag5.shape, 1) < 64, OMEGA / diag5, 0.0)
    u5 = scale5 * s5
    for _ in range(3):
        u5 = u5 + scale5 * (s5 - fluxes(u5, half5, fr5, fd5, 64, n // 4))
    e4 = double_rows(double_cols(u5, spread[:, :128]), scratch, u4.shape[0])
    u4 = u4 + e4 * 4.0
    u4 = u4 + scale4 * (s4 - fluxes(u4, half4, fr4, fd4, 128, n // 2))
    u3 = u3 + double_rows(double_cols(u4, spread), scratch, u3.shape[0]) * 4.0
    u3 = u3 + scale3 * (s3 - fluxes(u3, half3, fr3, fd3, 256, n))
    v3 = u3 * 64.0

    lane = iota((1, 128), 1)
    quantity = jnp.sum(gathered[pl.ds(6 * fields, slabs, stride=ROWS), :], axis=0, keepdims=True)
    both = w3 * v3
    both = both[:, :128] + both[:, 128:]
    for f in range(fields):
        quantity = quantity + jnp.where(lane == f, 64.0 * jnp.sum(both[f * n : (f + 1) * n]), 0.0)
    quantity = quantity / cells
    diffs = jnp.where(lane < slots, quantity - pltpu.roll(quantity, 128 - slots, 1), 0.0)
    live = lane < counts[0]
    counted = counts[0].astype(F32)
    mean = jnp.sum(jnp.where(live, diffs, 0.0), axis=1, keepdims=True) / counted
    spare = jnp.where(live, diffs - mean, 0.0)
    var = jnp.sum(spare * spare, axis=1, keepdims=True) / jnp.maximum(counted - 1.0, 1.0)
    stats[...] = jnp.zeros_like(stats)
    stats[0:1, :] = diffs
    stats[1:2, :] = jnp.where(lane == 0, mean, jnp.where(lane == 1, var, 0.0))
    sent = jnp.where(lane == 0, mean, jnp.where(lane == 1, var / counted, 0.0))
    for i in range(message.shape[0]):
        message[i] = jnp.broadcast_to(sent, (8, 128))

    whole[...] = jnp.zeros_like(whole)
    whole[8 : 8 + slots * n, :] = v3[: slots * n]
    e3[...] = jnp.zeros_like(e3)
    me = place[0]
    for f in range(slots):
        for r in range(3):
            line = whole[pl.ds(8 + f * n + me + (r - 1), 1), :]
            if r == 0:
                line = jnp.where(me > 0, line, 0.0)
            if r == 2:
                line = jnp.where(me < n - 1, line, 0.0)
            e3[f * 8 + r : f * 8 + r + 1, :] = line


def up_kernel(edge, kf, kfu, kfd, g, v0, v1, v2, s1, s2, k1, k2, e3, above, below_rows, out, scratch):
    spread = pair_matrix((128, 256), 1, 1.0)
    slots = kf.shape[0]

    def body(slot, _):
        row = iota((8, v2.shape[2]), 0)
        v = jnp.where(row == 0, above[pl.ds(slot, 1), :], jnp.where(row == 5, below_rows[pl.ds(slot, 1), :], v2[slot]))
        e = e3[pl.ds(pl.multiple_of(slot * 8, 8), 8), :]
        zero = jnp.zeros_like(g[...])
        for depth, k, s, v in (
            (2, k2[slot], s2[slot], v),
            (1, k1[slot], s1[slot], v1[slot]),
            (0, jnp.concatenate([kfu[slot], kf[slot], kfd[slot]], axis=0), jnp.concatenate([zero, g[...], zero], axis=0), v0[slot]),
        ):
            rows, cols = k.shape
            inside = row_mask(k.shape, depth, edge)
            v = jnp.where(inside, v + double_rows(double_cols(e, spread), scratch, rows), 0.0)
            half, fr, fd, diag = faces(k, cols, None)
            e = v + OMEGA * (s * (4.0**depth) - fluxes(v, half, fr, fd, cols, None)) / diag
            e = jnp.where(inside, e, 0.0)
            if depth == 1:
                e = e[:16]
        out[slot] = e[8:16]
        return 0

    lax.fori_loop(0, slots, body, 0)


def sum_kernel(got, out):
    total = got[0]
    for i in range(1, got.shape[0]):
        total = total + got[i]
    out[...] = total


VMEM = pl.BlockSpec(memory_space=pltpu.VMEM)
SMEM = pl.BlockSpec(memory_space=pltpu.SMEM)


def shape(*dims):
    return jax.ShapeDtypeStruct(dims, F32)


def call(kernel, outs, smem, vmem, scratch, flops, name, mib):
    single = not isinstance(outs, (tuple, list))
    return pl.pallas_call(
        kernel,
        out_shape=outs,
        in_specs=[SMEM] * len(smem) + [VMEM] * len(vmem),
        out_specs=VMEM if single else [VMEM] * len(outs),
        scratch_shapes=scratch,
        compiler_params=pltpu.CompilerParams(vmem_limit_bytes=mib << 20),
        cost_estimate=pl.CostEstimate(flops=flops, bytes_accessed=1 << 20, transcendentals=0),
        name=name,
    )(*smem, *vmem)


def on_device(coef_fine, coef_coarse, rhs_field, level_counts):
    slots, rows, cols = coef_fine.shape
    fields = 2 * slots
    outer, inner = lax.axis_size("slab_0"), lax.axis_size("slab_1")
    levels = lax.axis_size("level")
    slabs = outer * inner
    me = lax.axis_index(SLAB)
    from_above = [(i, i + 1) for i in range(slabs - 1)]
    from_below = [(i + 1, i) for i in range(slabs - 1)]
    kfu = lax.ppermute(coef_fine, SLAB, from_above)
    kfd = lax.ppermute(coef_fine, SLAB, from_below)
    gu = lax.ppermute(rhs_field, SLAB, from_above)
    gd = lax.ppermute(rhs_field, SLAB, from_below)
    kcu = lax.ppermute(coef_coarse, SLAB, from_above)
    kcd = lax.ppermute(coef_coarse, SLAB, from_below)
    edge = jnp.stack([jnp.where(me == 0, 8, 0), jnp.where(me == slabs - 1, 16, 24)]).astype(jnp.int32)
    place = me.astype(jnp.int32).reshape(1)

    packed, v0, v1, v2, s1, s2, k1, k2, to_below, to_above = call(
        down_kernel,
        [
            shape(inner, ROWS, 128),
            shape(slots, 24, cols),
            shape(slots, 16, cols // 2),
            shape(slots, 8, cols // 4),
            shape(slots, 16, cols // 2),
            shape(slots, 8, cols // 4),
            shape(slots, 16, cols // 2),
            shape(slots, 8, cols // 4),
            shape(8, cols // 4),
            shape(8, cols // 4),
        ],
        [edge],
        [coef_fine, coef_coarse, rhs_field, kfu, kcu, gu, kfd, kcd, gd],
        [pltpu.VMEM((cols // 4, 128), F32), pltpu.VMEM((fields * 8, 128), F32)],
        20_000_000,
        "down",
        24,
    )
    lines = lax.all_to_all(packed, "slab_1", 0, 0, tiled=True)
    above = lax.ppermute(to_below, SLAB, from_above)
    below_rows = lax.ppermute(to_above, SLAB, from_below)
    wide = jnp.broadcast_to(lines.reshape(1, inner * ROWS, 128), (outer, inner * ROWS, 128))
    gathered = lax.all_to_all(wide, "slab_0", 0, 0, tiled=True).reshape(slabs * ROWS, 128)
    e3, stats, message = call(
        functools.partial(coarse_kernel, slots=slots, slabs=slabs, cells=float(rows * slabs * cols)),
        [shape(slots * 8, 256), shape(8, 128), shape(levels, 8, 128)],
        [place, level_counts],
        [gathered],
        [pltpu.VMEM((2 * fields * slabs, 128), F32), pltpu.VMEM((slots * slabs + 16, 256), F32)],
        5_000_000,
        "coarse",
        16,
    )
    got = lax.all_to_all(message, "level", 0, 0, tiled=True)
    solutions = call(
        up_kernel,
        shape(slots, rows, cols),
        [edge],
        [coef_fine, kfu, kfd, rhs_field, v0, v1, v2, s1, s2, k1, k2, e3, above, below_rows],
        [pltpu.VMEM((cols // 4, 128), F32)],
        10_000_000,
        "up",
        24,
    )
    total = call(sum_kernel, shape(8, 128), [], [got], [], 1_000, "total", 4)
    return solutions, stats[0, :slots], stats[1:2, :2], total[0, :2]


def solution(mesh):
    slabs = mesh.shape["slab"]
    outer = 4 if slabs >= 64 else 2
    split = Mesh(mesh.devices.reshape(mesh.shape["level"], outer, slabs // outer), ("level", "slab_0", "slab_1"))
    in_specs = (P("level", SLAB, None), P("level", SLAB, None), P(SLAB, None), P("level"))
    out_specs = (P("level", SLAB, None), P("level"), P("level", None), P())
    return jax.shard_map(on_device, mesh=split, in_specs=in_specs, out_specs=out_specs, check_vma=False)
```

```python
import functools

import jax
import jax.numpy as jnp
from jax import lax
from jax.experimental import pallas as pl
from jax.experimental.pallas import tpu as pltpu
from jax.sharding import Mesh
from jax.sharding import PartitionSpec as P

OMEGA = 0.8
SLAB = ("slab_0", "slab_1")
LINES = 40
F32 = jnp.float32


def iota(shape, dim):
    return lax.broadcasted_iota(jnp.int32, shape, dim)


def right_of(x, cols):
    n = x.shape[1]
    return jnp.where(iota(x.shape, 1) == cols - 1, 0.0, pltpu.roll(x, n - 1, 1))


def below(x, period):
    n = x.shape[0]
    shifted = pltpu.roll(x, n - 1, 0)
    if period is None:
        return shifted
    return jnp.where(iota(x.shape, 0) % period == period - 1, 0.0, shifted)


def faces(k, cols, period):
    half = 0.5 * k
    first = iota(k.shape, 1) == 0
    fr = half + right_of(half, cols)
    fl = jnp.where(first, half, pltpu.roll(fr, 1, 1))
    fd = half + below(half, period)
    fu = pltpu.roll(fd, 1, 0)
    if period is not None:
        fu = jnp.where(iota(k.shape, 0) % period == 0, half, fu)
    return half, fr, fd, (fr + fl) + (fd + fu)


def across(u, half, fr, cols):
    q = fr * (u - right_of(u, cols))
    return q - jnp.where(iota(u.shape, 1) == 0, -half * u, pltpu.roll(q, 1, 1))


def fluxes(u, half, fr, fd, cols, period):
    p = fd * (u - below(u, period))
    pu = pltpu.roll(p, 1, 0)
    if period is not None:
        pu = jnp.where(iota(u.shape, 0) % period == 0, -half * u, pu)
    return across(u, half, fr, cols) + (p - pu)


def pair_matrix(shape, dim, value):
    long, short = iota(shape, dim), iota(shape, 1 - dim)
    return jnp.where(long // 2 == short, value, 0.0).astype(jnp.bfloat16)


def dot(a, b):
    high = a.astype(jnp.bfloat16)
    rest = a - high.astype(F32)
    middle = rest.astype(jnp.bfloat16)
    low = (rest - middle.astype(F32)).astype(jnp.bfloat16)
    one = functools.partial(jnp.dot, preferred_element_type=F32)
    return one(high, b) + (one(middle, b) + one(low, b))


def pieces(x, width=128):
    return [x[:, i : i + width] for i in range(0, x.shape[1], width)]


def pairs_of_rows(x, scratch):
    rows = x.shape[0]
    room = -(-rows // 16) * 16
    parts = pieces(x)
    for i, piece in enumerate(parts):
        scratch[i * room : i * room + rows, :] = piece
    out = len(parts) * room // 2
    return scratch[pl.ds(0, out, stride=2), :] + scratch[pl.ds(1, out, stride=2), :], room // 2


def halve(x, scratch, quarter):
    tall, rows = pairs_of_rows(x, scratch)
    n = x.shape[1] // 128
    blocks = [tall[i * rows : (i + 1) * rows] for i in range(n)]
    if n == 1:
        return dot(tall, quarter[:128])
    both = jnp.concatenate(
        [jnp.concatenate(blocks[0::2], axis=0), jnp.concatenate(blocks[1::2], axis=0)], axis=1
    )
    got = dot(both, quarter)
    return jnp.concatenate([got[i * rows : (i + 1) * rows] for i in range(n // 2)], axis=1)


def double_cols(x, spread):
    rows = x.shape[0]
    parts = pieces(x)
    got = dot(jnp.concatenate(parts, axis=0), spread)
    return jnp.concatenate([got[i * rows : (i + 1) * rows] for i in range(len(parts))], axis=1)


def double_rows(x, scratch):
    rows = x.shape[0]
    parts = pieces(x)
    for i, piece in enumerate(parts):
        scratch[pl.ds(i * 2 * rows, rows, stride=2), :] = piece
        scratch[pl.ds(i * 2 * rows + 1, rows, stride=2), :] = piece
    return jnp.concatenate([scratch[i * 2 * rows : (i + 1) * 2 * rows, :] for i in range(len(parts))], axis=1)


def inside(shape, depth, edge, window):
    row = iota(shape, 0) % window
    return (row >= (edge[0] >> depth)) & (row < (edge[1] >> depth))


def summed(parts):
    return functools.reduce(jnp.add, parts)


def sweep(k, s, w, depth, window, edge):
    cols = k.shape[1]
    half, fr, fd, diag = faces(k, cols, None)
    scale = jnp.where(inside(k.shape, depth, edge, window), OMEGA / diag, 0.0)
    us = scale * s
    uw = scale if w is None else scale * w
    rs = s - fluxes(us, half, fr, fd, cols, None)
    rw = (1.0 if w is None else w) - fluxes(uw, half, fr, fd, cols, None)
    return us, rs, rw, rw * us + uw * s


def down_kernel(
    edge, here, above, under,
    packed, rims, s1_out, s2_out, k1_out, k2_out, to_below, to_above,
    scratch, even, odd, parts,
):
    quarter = pair_matrix((256, 128), 0, 0.25)
    fields = here.shape[0] - 1
    slots = fields // 2
    copies = packed.shape[0]
    chunks = here.shape[2] // 128
    source = jnp.concatenate([above[fields], here[fields], under[fields]], axis=0)
    for q in range(3):
        for i in range(chunks):
            scratch[q, i * 32 + 24 : i * 32 + 32, :] = jnp.zeros((8, 128), F32)

    def finest(fine, field, _):
        k = jnp.concatenate([above[field], here[field], under[field]], axis=0)
        us, rs, rw, share = sweep(k, source, None, 0, 24, edge)
        parts[pl.ds(pl.multiple_of(field * 8, 8), 8), :] = summed(pieces(share[8:16]))
        if fine:
            rims[field, 0:1, :] = k[7:8]
            rims[field, 1:2, :] = k[16:17]
            rims[field, 2:3, :] = us[7:8]
            rims[field, 3:4, :] = us[16:17]
        for q, x in enumerate((k, rs, rw)):
            tall, rows = pairs_of_rows(x, scratch.at[q])
            for i in range(chunks):
                into = even if i % 2 == 0 else odd
                at = pl.multiple_of((q * (chunks // 2) + i // 2) * fields * rows + field * rows, 8)
                into[pl.ds(at, rows), :] = tall[i * rows : (i + 1) * rows]
        return 0

    lax.fori_loop(0, slots, functools.partial(finest, True), 0)
    lax.fori_loop(slots, fields, functools.partial(finest, False), 0)

    block = fields * 16
    level = []
    for q in range(3):
        span = slice(q * (chunks // 2) * block, (q + 1) * (chunks // 2) * block)
        got = dot(jnp.concatenate([even[span, :], odd[span, :]], axis=1), quarter)
        level.append(jnp.concatenate([got[i * block : (i + 1) * block] for i in range(chunks // 2)], axis=1))
    for depth, window in ((1, 16), (2, 8)):
        k, s, w = level
        us, rs, rw, share = sweep(k, s, w, depth, window, edge)
        own = 8 >> depth
        row = iota(share.shape, 0) % window
        share = summed(pieces(jnp.where((row >= own) & (row < 2 * own), share, 0.0))) * (16.0**depth)
        for field in range(fields):
            at = field * window
            parts[field * 8 : field * 8 + 8, :] += summed([share[at + i : at + i + 8] for i in range(0, window, 8)])
        kept = slots * window
        if depth == 1:
            s1_out[...], k1_out[...] = s[:kept], k[:kept]
        else:
            s2_out[...], k2_out[...] = s[:kept], k[:kept]
            to_below[...] = jnp.zeros_like(to_below)
            to_above[...] = jnp.zeros_like(to_above)
            for slot in range(slots):
                to_below[slot : slot + 1, :] = us[slot * 8 + 2 : slot * 8 + 3] * 16.0
                to_above[slot : slot + 1, :] = us[slot * 8 + 3 : slot * 8 + 4] * 16.0
        level = [halve(x, scratch.at[q], quarter) for q, x in enumerate((k, rs, rw))]

    for q, x in enumerate(level):
        for field in range(fields):
            for h in range(2):
                line = x[field * 4 + 1 : field * 4 + 2, h * 128 : (h + 1) * 128]
                packed[0, (q * fields + field) * 2 + h : (q * fields + field) * 2 + h + 1, :] = line
    lane = iota((1, 128), 1)
    line = jnp.zeros((1, 128), F32)
    for field in range(fields):
        line = line + jnp.where(lane == field, jnp.sum(parts[field * 8 : field * 8 + 8, :]), 0.0)
    packed[0, 6 * fields : 6 * fields + 1, :] = line
    packed[0, 6 * fields + 1 :, :] = jnp.zeros((LINES - 6 * fields - 1, 128), F32)
    for i in range(1, copies):
        packed[i] = packed[0]


def coarse_kernel(place, counts, gathered, lines, top, bottom, e3, message, scratch, whole, *, fields, slabs, rows, cells):
    del top, bottom
    slots = fields // 2
    quarter = pair_matrix((256, 128), 0, 0.25)
    spread = pair_matrix((128, 256), 1, 1.0)
    stride = 4 * fields
    n = slabs

    def taken(q):
        halves = [
            jnp.concatenate(
                [gathered[pl.ds((q * fields + f) * 2 + h, n, stride=stride), :] for f in range(fields)], axis=0
            )
            for h in range(2)
        ]
        return jnp.concatenate(halves, axis=1)

    k3, s3 = taken(0), taken(1)
    half3, fr3, fd3, diag3 = faces(k3, 256, n)
    scale3 = OMEGA / diag3
    u3 = scale3 * s3
    k4 = halve(k3, scratch.at[0], quarter)
    s4 = halve(s3 - fluxes(u3, half3, fr3, fd3, 256, n), scratch.at[1], quarter)
    half4, fr4, fd4, diag4 = faces(k4, 128, n // 2)
    scale4 = OMEGA / diag4
    u4 = scale4 * s4
    k5 = halve(k4, scratch.at[0], quarter)
    s5 = halve(s4 - fluxes(u4, half4, fr4, fd4, 128, n // 2), scratch.at[1], quarter)
    half5, fr5, fd5, diag5 = faces(k5, 64, n // 4)
    scale5 = jnp.where(iota(diag5.shape, 1) < 64, OMEGA / diag5, 0.0)
    u5 = scale5 * s5
    for _ in range(3):
        u5 = u5 + scale5 * (s5 - fluxes(u5, half5, fr5, fd5, 64, n // 4))
    u4 = u4 + double_rows(double_cols(u5, spread[:, :128]), scratch.at[0]) * 4.0
    u4 = u4 + scale4 * (s4 - fluxes(u4, half4, fr4, fd4, 128, n // 2))
    u3 = u3 + double_rows(double_cols(u4, spread), scratch.at[0]) * 4.0
    u3 = u3 + scale3 * (s3 - fluxes(u3, half3, fr3, fd3, 256, n))
    v3 = u3 * 64.0
    whole[0:8, :] = jnp.zeros((8, 256), F32)
    whole[8 : 8 + fields * n, :] = v3
    whole[8 + fields * n :, :] = jnp.zeros((8, 256), F32)

    lane = iota((1, 128), 1)
    block = pl.multiple_of(place[1] * rows, 8)

    def weighed(f):
        v = whole[pl.ds(8 + f * n + block, rows), :]
        w = [lines[pl.ds((2 * fields + f) * 2 + h, rows, stride=LINES), :] for h in range(2)]
        return v[:, :128] * w[0] + v[:, 128:] * w[1]

    total = jnp.sum(lines[pl.ds(6 * fields, rows, stride=LINES), :], axis=0, keepdims=True)
    total = total - pltpu.roll(total, 128 - slots, 1)
    for f in range(slots):
        total = total + jnp.where(lane == f, 64.0 * jnp.sum(weighed(f) - weighed(slots + f)), 0.0)
    sent = jnp.where(lane < slots, total / cells, jnp.where(lane == slots, counts[0].astype(F32), 0.0))
    sent = jnp.broadcast_to(sent, (8, 128))
    for i in range(message.shape[0]):
        message[i] = sent

    me = place[0]
    e3[...] = jnp.zeros_like(e3)
    for f in range(slots):
        for r in range(3):
            line = whole[pl.ds(8 + f * n + me + (r - 1), 1), :]
            if r == 0:
                line = jnp.where(me > 0, line, 0.0)
            if r == 2:
                line = jnp.where(me < n - 1, line, 0.0)
            e3[f * 8 + r : f * 8 + r + 1, :] = line


def up_kernel(edge, here, g, rims, s1, s2, k1, k2, e3, top, bottom, out, scratch):
    spread = pair_matrix((128, 256), 1, 1.0)
    slots = here.shape[0]

    def relaxed(k, s, e, depth, window, swap):
        half, fr, fd, diag = faces(k, k.shape[1], None)
        scale = OMEGA / diag
        s = s * (4.0**depth)
        valid = inside(k.shape, depth, edge, window)
        v = jnp.where(valid, swap(scale * s) + e, 0.0)
        return jnp.where(valid, v + scale * (s - fluxes(v, half, fr, fd, k.shape[1], None)), 0.0)

    def stacked(ref, rows):
        return jnp.concatenate([jnp.broadcast_to(ref[f : f + 1, :], (rows, ref.shape[1])) for f in range(slots)], axis=0)

    def rimmed(v):
        row = iota(v.shape, 0) % 8
        return jnp.where(row == 0, stacked(top, 8), jnp.where(row == 5, stacked(bottom, 8), v))

    e = double_rows(double_cols(e3[...], spread), scratch)
    e = jnp.concatenate([e[f * 16 : f * 16 + 8] for f in range(slots)], axis=0)
    e = relaxed(k2[...], s2[...], e, 2, 8, rimmed)
    e = double_rows(double_cols(e, spread), scratch)
    e = relaxed(k1[...], s1[...], e, 1, 16, lambda v: v)
    e = double_cols(e, spread)
    g = g[...]
    row = iota(g.shape, 0)
    cols = g.shape[1]

    def lower(x, last):
        return jnp.where(row == 7, last, pltpu.roll(x, 7, 0))

    def upper(x, first):
        return jnp.where(row == 0, first, pltpu.roll(x, 1, 0))

    for f in range(slots):
        k = here[f]
        half = 0.5 * k
        fr = half + right_of(half, cols)
        fl = jnp.where(iota(k.shape, 1) == 0, half, pltpu.roll(fr, 1, 1))
        fd = half + lower(half, 0.5 * rims[f, 1:2, :])
        fu = half + upper(half, 0.5 * rims[f, 0:1, :])
        scale = OMEGA / ((fr + fl) + (fd + fu))
        at = f * 16
        v = scale * g + double_rows(e[at : at + 8], scratch)[8:16]
        first = rims[f, 2:3, :] + e[at + 3 : at + 4]
        last = rims[f, 3:4, :] + e[at + 8 : at + 9]
        flow = across(v, half, fr, cols) + (fd * (v - lower(v, last)) + fu * (v - upper(v, first)))
        out[f] = v + scale * (g - flow)


def final_kernel(place, got, diffs, moments, estimate, *, levels, outer):
    slots = diffs.shape[0]
    row, lane = iota((8, 128), 0), iota((8, 128), 1)
    table = jnp.zeros((8, 128), F32)
    for m in range(levels):
        table = jnp.where(row == m, summed([got[m * outer + i] for i in range(outer)]), table)

    def along(x):
        return jnp.sum(x, axis=1, keepdims=True)

    counted = along(jnp.where(lane == slots, table, 0.0)) / outer
    counted = jnp.where(row[:, :1] < levels, counted, 1.0)
    live = (lane < slots) & (lane.astype(F32) < counted) & (row < levels)
    mean = along(jnp.where(live, table, 0.0)) / counted
    spare = jnp.where(live, table - mean, 0.0)
    var = along(spare * spare) / jnp.maximum(counted - 1.0, 1.0)
    both = jnp.where(lane == 0, mean, jnp.where(lane == 1, var, 0.0))
    sums = jnp.where(lane == 0, mean, jnp.where(lane == 1, var / counted, 0.0))
    sums = jnp.sum(sums, axis=0, keepdims=True)
    mine = row == place[2]
    own = jnp.sum(jnp.where(mine, table, 0.0), axis=0, keepdims=True)
    both = jnp.sum(jnp.where(mine, both, 0.0), axis=0, keepdims=True)
    for i in range(slots):
        diffs[i] = own[0, i]
    for i in range(2):
        moments[0, i] = both[0, i]
        estimate[i] = sums[0, i]


VMEM = pl.BlockSpec(memory_space=pltpu.VMEM)
SMEM = pl.BlockSpec(memory_space=pltpu.SMEM)


def shape(*dims):
    return jax.ShapeDtypeStruct(dims, F32)


def call(kernel, outs, smem, vmem, scratch, flops, name, mib, scalars=0):
    return pl.pallas_call(
        kernel,
        out_shape=outs,
        in_specs=[SMEM] * len(smem) + [VMEM] * len(vmem),
        out_specs=[VMEM] * (len(outs) - scalars) + [SMEM] * scalars,
        scratch_shapes=[pltpu.VMEM(s, F32) for s in scratch],
        compiler_params=pltpu.CompilerParams(vmem_limit_bytes=mib << 20),
        cost_estimate=pl.CostEstimate(flops=flops, bytes_accessed=1 << 20, transcendentals=0),
        name=name,
    )(*smem, *vmem)


def on_device(coef_fine, coef_coarse, rhs_field, level_counts):
    slots, rows, cols = coef_fine.shape
    fields = 2 * slots
    outer, inner = lax.axis_size("slab_0"), lax.axis_size("slab_1")
    levels = lax.axis_size("level")
    slabs = outer * inner
    me = lax.axis_index(SLAB)
    from_above = [(i, i + 1) for i in range(slabs - 1)]
    from_below = [(i + 1, i) for i in range(slabs - 1)]
    here = jnp.concatenate([coef_fine, coef_coarse, rhs_field[None]], axis=0)
    above = lax.ppermute(here, SLAB, from_above)
    under = lax.ppermute(here, SLAB, from_below)
    edge = jnp.stack([jnp.where(me == 0, 8, 0), jnp.where(me == slabs - 1, 16, 24)]).astype(jnp.int32)
    place = jnp.stack([me, lax.axis_index("slab_0"), lax.axis_index("level")]).astype(jnp.int32)

    packed, rims, s1, s2, k1, k2, to_below, to_above = call(
        down_kernel,
        [
            shape(inner, LINES, 128),
            shape(slots, 8, cols),
            shape(slots * 16, cols // 2),
            shape(slots * 8, cols // 4),
            shape(slots * 16, cols // 2),
            shape(slots * 8, cols // 4),
            shape(8, cols // 4),
            shape(8, cols // 4),
        ],
        [edge],
        [here, above, under],
        [
            (3, max(cols // 4, 768), 128),
            (3 * fields * cols // 16, 128),
            (3 * fields * cols // 16, 128),
            (fields * 8, 128),
        ],
        20_000_000,
        "down",
        28,
    )
    lines = lax.all_to_all(packed, "slab_1", 0, 0, tiled=True)
    lines, to_below, to_above = lax.optimization_barrier((lines, to_below, to_above))
    top = lax.ppermute(to_below, SLAB, from_above)
    bottom = lax.ppermute(to_above, SLAB, from_below)
    used = 4 * fields
    wide = jnp.broadcast_to(lines[None, :, :used], (outer, inner, used, 128))
    gathered = lax.all_to_all(wide, "slab_0", 0, 0, tiled=True).reshape(slabs * used, 128)
    e3, message = call(
        functools.partial(coarse_kernel, fields=fields, slabs=slabs, rows=inner, cells=float(rows * slabs * cols)),
        [shape(slots * 8, 256), shape(levels * outer, 8, 128)],
        [place, level_counts],
        [gathered, lines.reshape(inner * LINES, 128), top, bottom],
        [(2, 2 * fields * slabs, 128), (fields * slabs + 16, 256)],
        5_000_000,
        "coarse",
        16,
    )
    got = lax.all_to_all(message, ("level", "slab_0"), 0, 0, tiled=True)
    (solutions,) = call(
        up_kernel,
        [shape(slots, rows, cols)],
        [edge],
        [coef_fine, rhs_field, rims, s1, s2, k1, k2, e3, top, bottom],
        [(cols // 2, 128)],
        10_000_000,
        "up",
        16,
    )
    diffs, moments, estimate = call(
        functools.partial(final_kernel, levels=levels, outer=outer),
        [shape(slots), shape(1, 2), shape(2)],
        [place],
        [got],
        [],
        1_000,
        "final",
        4,
        3,
    )
    return solutions, diffs, moments, estimate


def solution(mesh):
    slabs = mesh.shape["slab"]
    outer = 4 if slabs >= 64 else 2
    split = Mesh(mesh.devices.reshape(mesh.shape["level"], outer, slabs // outer), ("level", "slab_0", "slab_1"))
    in_specs = (P("level", SLAB, None), P("level", SLAB, None), P(SLAB, None), P("level"))
    out_specs = (P("level", SLAB, None), P("level"), P("level", None), P())
    return jax.shard_map(on_device, mesh=split, in_specs=in_specs, out_specs=out_specs, check_vma=False)
```

```python
import functools

import jax
import jax.numpy as jnp
from jax import lax
from jax.experimental import pallas as pl
from jax.experimental.pallas import tpu as pltpu
from jax.sharding import Mesh
from jax.sharding import PartitionSpec as P

OMEGA = 0.8
SLAB = ("slab_0", "slab_1")
LINES = 40
F32 = jnp.float32


def iota(shape, dim):
    return lax.broadcasted_iota(jnp.int32, shape, dim)


def right_of(x, cols):
    n = x.shape[1]
    return jnp.where(iota(x.shape, 1) == cols - 1, 0.0, pltpu.roll(x, n - 1, 1))


def below(x, period):
    n = x.shape[0]
    shifted = pltpu.roll(x, n - 1, 0)
    if period is None:
        return shifted
    return jnp.where(iota(x.shape, 0) % period == period - 1, 0.0, shifted)


def faces(k, cols, period):
    half = 0.5 * k
    first = iota(k.shape, 1) == 0
    fr = half + right_of(half, cols)
    fl = jnp.where(first, half, pltpu.roll(fr, 1, 1))
    fd = half + below(half, period)
    fu = pltpu.roll(fd, 1, 0)
    if period is not None:
        fu = jnp.where(iota(k.shape, 0) % period == 0, half, fu)
    return half, fr, fd, (fr + fl) + (fd + fu)


def across(u, half, fr, cols):
    q = fr * (u - right_of(u, cols))
    return q - jnp.where(iota(u.shape, 1) == 0, -half * u, pltpu.roll(q, 1, 1))


def fluxes(u, half, fr, fd, cols, period):
    p = fd * (u - below(u, period))
    pu = pltpu.roll(p, 1, 0)
    if period is not None:
        pu = jnp.where(iota(u.shape, 0) % period == 0, -half * u, pu)
    return across(u, half, fr, cols) + (p - pu)


def pair_matrix(shape, dim, value):
    long, short = iota(shape, dim), iota(shape, 1 - dim)
    return jnp.where(long // 2 == short, value, 0.0).astype(jnp.bfloat16)


def dot(a, b):
    high = a.astype(jnp.bfloat16)
    rest = a - high.astype(F32)
    middle = rest.astype(jnp.bfloat16)
    low = (rest - middle.astype(F32)).astype(jnp.bfloat16)
    one = functools.partial(jnp.dot, preferred_element_type=F32)
    return one(high, b) + (one(middle, b) + one(low, b))


def pieces(x, width=128):
    return [x[:, i : i + width] for i in range(0, x.shape[1], width)]


def pairs_of_rows(x, scratch):
    rows = x.shape[0]
    room = -(-rows // 16) * 16
    parts = pieces(x)
    for i, piece in enumerate(parts):
        scratch[i * room : i * room + rows, :] = piece
    out = len(parts) * room // 2
    return scratch[pl.ds(0, out, stride=2), :] + scratch[pl.ds(1, out, stride=2), :], room // 2


def halve(x, scratch, quarter):
    tall, rows = pairs_of_rows(x, scratch)
    n = x.shape[1] // 128
    blocks = [tall[i * rows : (i + 1) * rows] for i in range(n)]
    if n == 1:
        return dot(tall, quarter[:128])
    both = jnp.concatenate(
        [jnp.concatenate(blocks[0::2], axis=0), jnp.concatenate(blocks[1::2], axis=0)], axis=1
    )
    got = dot(both, quarter)
    return jnp.concatenate([got[i * rows : (i + 1) * rows] for i in range(n // 2)], axis=1)


def double_cols(x, spread):
    rows = x.shape[0]
    parts = pieces(x)
    got = dot(jnp.concatenate(parts, axis=0), spread)
    return jnp.concatenate([got[i * rows : (i + 1) * rows] for i in range(len(parts))], axis=1)


def double_rows(x, scratch):
    rows = x.shape[0]
    parts = pieces(x)
    for i, piece in enumerate(parts):
        scratch[pl.ds(i * 2 * rows, rows, stride=2), :] = piece
        scratch[pl.ds(i * 2 * rows + 1, rows, stride=2), :] = piece
    return jnp.concatenate([scratch[i * 2 * rows : (i + 1) * 2 * rows, :] for i in range(len(parts))], axis=1)


def inside(shape, depth, edge, window):
    row = iota(shape, 0) % window
    return (row >= (edge[0] >> depth)) & (row < (edge[1] >> depth))


def summed(parts):
    return functools.reduce(jnp.add, parts)


def sweep(k, s, w, depth, window, edge):
    cols = k.shape[1]
    half, fr, fd, diag = faces(k, cols, None)
    scale = jnp.where(inside(k.shape, depth, edge, window), OMEGA / diag, 0.0)
    us = scale * s
    uw = scale if w is None else scale * w
    rs = s - fluxes(us, half, fr, fd, cols, None)
    rw = (1.0 if w is None else w) - fluxes(uw, half, fr, fd, cols, None)
    return us, rs, rw, rw * us + uw * s


def down_kernel(
    edge, here, one, two,
    packed, rims, s1_out, s2_out, k1_out, k2_out, to_below, to_above,
    scratch, even, odd, parts,
):
    quarter = pair_matrix((256, 128), 0, 0.25)
    fields = here.shape[0] - 1
    slots = fields // 2
    copies = packed.shape[0]
    chunks = here.shape[2] // 128
    flip = edge[2] == 1

    def window(at):
        a, b = one[at], two[at]
        return jnp.concatenate([jnp.where(flip, b, a), here[at], jnp.where(flip, a, b)], axis=0)

    source = window(fields)
    for q in range(3):
        for i in range(chunks):
            scratch[q, i * 32 + 24 : i * 32 + 32, :] = jnp.zeros((8, 128), F32)

    def finest(fine, field, _):
        k = window(field)
        us, rs, rw, share = sweep(k, source, None, 0, 24, edge)
        parts[pl.ds(pl.multiple_of(field * 8, 8), 8), :] = summed(pieces(share[8:16]))
        if fine:
            rims[field, 0:1, :] = k[7:8]
            rims[field, 1:2, :] = k[16:17]
            rims[field, 2:3, :] = us[7:8]
            rims[field, 3:4, :] = us[16:17]
        for q, x in enumerate((k, rs, rw)):
            tall, rows = pairs_of_rows(x, scratch.at[q])
            for i in range(chunks):
                into = even if i % 2 == 0 else odd
                at = pl.multiple_of((q * (chunks // 2) + i // 2) * fields * rows + field * rows, 8)
                into[pl.ds(at, rows), :] = tall[i * rows : (i + 1) * rows]
        return 0

    lax.fori_loop(0, slots, functools.partial(finest, True), 0)
    lax.fori_loop(slots, fields, functools.partial(finest, False), 0)

    block = fields * 16
    level = []
    for q in range(3):
        span = slice(q * (chunks // 2) * block, (q + 1) * (chunks // 2) * block)
        got = dot(jnp.concatenate([even[span, :], odd[span, :]], axis=1), quarter)
        level.append(jnp.concatenate([got[i * block : (i + 1) * block] for i in range(chunks // 2)], axis=1))
    for depth, room in ((1, 16), (2, 8)):
        k, s, w = level
        us, rs, rw, share = sweep(k, s, w, depth, room, edge)
        own = 8 >> depth
        row = iota(share.shape, 0) % room
        share = summed(pieces(jnp.where((row >= own) & (row < 2 * own), share, 0.0))) * (16.0**depth)
        for field in range(fields):
            at = field * room
            parts[field * 8 : field * 8 + 8, :] += summed([share[at + i : at + i + 8] for i in range(0, room, 8)])
        kept = slots * room
        if depth == 1:
            s1_out[...], k1_out[...] = s[:kept], k[:kept]
        else:
            s2_out[...], k2_out[...] = s[:kept], k[:kept]
            to_below[...] = jnp.zeros_like(to_below)
            to_above[...] = jnp.zeros_like(to_above)
            for slot in range(slots):
                to_below[slot : slot + 1, :] = us[slot * 8 + 2 : slot * 8 + 3] * 16.0
                to_above[slot : slot + 1, :] = us[slot * 8 + 3 : slot * 8 + 4] * 16.0
        level = [halve(x, scratch.at[q], quarter) for q, x in enumerate((k, rs, rw))]

    for q, x in enumerate(level):
        for field in range(fields):
            for h in range(2):
                line = x[field * 4 + 1 : field * 4 + 2, h * 128 : (h + 1) * 128]
                packed[0, (q * fields + field) * 2 + h : (q * fields + field) * 2 + h + 1, :] = line
    lane = iota((1, 128), 1)
    line = jnp.zeros((1, 128), F32)
    for field in range(fields):
        line = line + jnp.where(lane == field, jnp.sum(parts[field * 8 : field * 8 + 8, :]), 0.0)
    packed[0, 6 * fields : 6 * fields + 1, :] = line
    packed[0, 6 * fields + 1 :, :] = jnp.zeros((LINES - 6 * fields - 1, 128), F32)
    for i in range(1, copies):
        packed[i] = packed[0]


def coarse_kernel(place, counts, gathered, lines, top, bottom, e3, message, scratch, whole, *, fields, slabs, rows, cells):
    del top, bottom
    slots = fields // 2
    quarter = pair_matrix((256, 128), 0, 0.25)
    spread = pair_matrix((128, 256), 1, 1.0)
    stride = 4 * fields
    n = slabs

    def taken(q):
        halves = [
            jnp.concatenate(
                [gathered[pl.ds((q * fields + f) * 2 + h, n, stride=stride), :] for f in range(fields)], axis=0
            )
            for h in range(2)
        ]
        return jnp.concatenate(halves, axis=1)

    k3, s3 = taken(0), taken(1)
    half3, fr3, fd3, diag3 = faces(k3, 256, n)
    scale3 = OMEGA / diag3
    u3 = scale3 * s3
    k4 = halve(k3, scratch.at[0], quarter)
    s4 = halve(s3 - fluxes(u3, half3, fr3, fd3, 256, n), scratch.at[1], quarter)
    half4, fr4, fd4, diag4 = faces(k4, 128, n // 2)
    scale4 = OMEGA / diag4
    u4 = scale4 * s4
    k5 = halve(k4, scratch.at[0], quarter)
    s5 = halve(s4 - fluxes(u4, half4, fr4, fd4, 128, n // 2), scratch.at[1], quarter)
    half5, fr5, fd5, diag5 = faces(k5, 64, n // 4)
    scale5 = jnp.where(iota(diag5.shape, 1) < 64, OMEGA / diag5, 0.0)
    u5 = scale5 * s5
    for _ in range(3):
        u5 = u5 + scale5 * (s5 - fluxes(u5, half5, fr5, fd5, 64, n // 4))
    u4 = u4 + double_rows(double_cols(u5, spread[:, :128]), scratch.at[0]) * 4.0
    u4 = u4 + scale4 * (s4 - fluxes(u4, half4, fr4, fd4, 128, n // 2))
    u3 = u3 + double_rows(double_cols(u4, spread), scratch.at[0]) * 4.0
    u3 = u3 + scale3 * (s3 - fluxes(u3, half3, fr3, fd3, 256, n))
    v3 = u3 * 64.0
    whole[0:8, :] = jnp.zeros((8, 256), F32)
    whole[8 : 8 + fields * n, :] = v3
    whole[8 + fields * n :, :] = jnp.zeros((8, 256), F32)

    lane = iota((1, 128), 1)
    block = pl.multiple_of(place[1] * rows, 8)

    def weighed(f):
        v = whole[pl.ds(8 + f * n + block, rows), :]
        w = [lines[pl.ds((2 * fields + f) * 2 + h, rows, stride=LINES), :] for h in range(2)]
        return v[:, :128] * w[0] + v[:, 128:] * w[1]

    total = jnp.sum(lines[pl.ds(6 * fields, rows, stride=LINES), :], axis=0, keepdims=True)
    total = total - pltpu.roll(total, 128 - slots, 1)
    for f in range(slots):
        total = total + jnp.where(lane == f, 64.0 * jnp.sum(weighed(f) - weighed(slots + f)), 0.0)
    sent = jnp.where(lane < slots, total / cells, jnp.where(lane == slots, counts[0].astype(F32), 0.0))
    for i in range(message.shape[0]):
        message[i] = sent

    me = place[0]
    e3[...] = jnp.zeros_like(e3)
    for f in range(slots):
        for r in range(3):
            line = whole[pl.ds(8 + f * n + me + (r - 1), 1), :]
            if r == 0:
                line = jnp.where(me > 0, line, 0.0)
            if r == 2:
                line = jnp.where(me < n - 1, line, 0.0)
            e3[f * 8 + r : f * 8 + r + 1, :] = line


def up_kernel(edge, here, g, rims, s1, s2, k1, k2, e3, top, bottom, out, scratch):
    spread = pair_matrix((128, 256), 1, 1.0)
    slots = here.shape[0]

    def relaxed(k, s, e, depth, window, swap):
        half, fr, fd, diag = faces(k, k.shape[1], None)
        scale = OMEGA / diag
        s = s * (4.0**depth)
        valid = inside(k.shape, depth, edge, window)
        v = jnp.where(valid, swap(scale * s) + e, 0.0)
        return jnp.where(valid, v + scale * (s - fluxes(v, half, fr, fd, k.shape[1], None)), 0.0)

    def stacked(ref, rows):
        return jnp.concatenate([jnp.broadcast_to(ref[f : f + 1, :], (rows, ref.shape[1])) for f in range(slots)], axis=0)

    def rimmed(v):
        row = iota(v.shape, 0) % 8
        return jnp.where(row == 0, stacked(top, 8), jnp.where(row == 5, stacked(bottom, 8), v))

    e = double_rows(double_cols(e3[...], spread), scratch)
    e = jnp.concatenate([e[f * 16 : f * 16 + 8] for f in range(slots)], axis=0)
    e = relaxed(k2[...], s2[...], e, 2, 8, rimmed)
    e = double_rows(double_cols(e, spread), scratch)
    e = relaxed(k1[...], s1[...], e, 1, 16, lambda v: v)
    e = double_cols(e, spread)
    g = g[...]
    row = iota(g.shape, 0)
    cols = g.shape[1]

    def lower(x, last):
        return jnp.where(row == 7, last, pltpu.roll(x, 7, 0))

    def upper(x, first):
        return jnp.where(row == 0, first, pltpu.roll(x, 1, 0))

    for f in range(slots):
        k = here[f]
        half = 0.5 * k
        fr = half + right_of(half, cols)
        fl = jnp.where(iota(k.shape, 1) == 0, half, pltpu.roll(fr, 1, 1))
        fd = half + lower(half, 0.5 * rims[f, 1:2, :])
        fu = half + upper(half, 0.5 * rims[f, 0:1, :])
        scale = OMEGA / ((fr + fl) + (fd + fu))
        at = f * 16
        v = scale * g + double_rows(e[at : at + 8], scratch)[8:16]
        first = rims[f, 2:3, :] + e[at + 3 : at + 4]
        last = rims[f, 3:4, :] + e[at + 8 : at + 9]
        flow = across(v, half, fr, cols) + (fd * (v - lower(v, last)) + fu * (v - upper(v, first)))
        out[f] = v + scale * (g - flow)


def final_kernel(place, got, diffs, moments, estimate, *, levels, outer):
    slots = diffs.shape[0]
    row, lane = iota((8, 128), 0), iota((8, 128), 1)
    table = jnp.zeros((8, 128), F32)
    for m in range(levels):
        table = jnp.where(row == m, summed([got[m * outer + i] for i in range(outer)]), table)

    def along(x):
        return jnp.sum(x, axis=1, keepdims=True)

    counted = along(jnp.where(lane == slots, table, 0.0)) / outer
    counted = jnp.where(row[:, :1] < levels, counted, 1.0)
    live = (lane < slots) & (lane.astype(F32) < counted) & (row < levels)
    mean = along(jnp.where(live, table, 0.0)) / counted
    spare = jnp.where(live, table - mean, 0.0)
    var = along(spare * spare) / jnp.maximum(counted - 1.0, 1.0)
    both = jnp.where(lane == 0, mean, jnp.where(lane == 1, var, 0.0))
    sums = jnp.where(lane == 0, mean, jnp.where(lane == 1, var / counted, 0.0))
    sums = jnp.sum(sums, axis=0, keepdims=True)
    mine = row == place[2]
    own = jnp.sum(jnp.where(mine, table, 0.0), axis=0, keepdims=True)
    both = jnp.sum(jnp.where(mine, both, 0.0), axis=0, keepdims=True)
    for i in range(slots):
        diffs[i] = own[0, i]
    for i in range(2):
        moments[0, i] = both[0, i]
        estimate[i] = sums[0, i]


VMEM = pl.BlockSpec(memory_space=pltpu.VMEM)
SMEM = pl.BlockSpec(memory_space=pltpu.SMEM)


def shape(*dims):
    return jax.ShapeDtypeStruct(dims, F32)


def call(kernel, outs, smem, vmem, scratch, flops, mib, scalars=0):
    return pl.pallas_call(
        kernel,
        out_shape=outs,
        in_specs=[SMEM] * len(smem) + [VMEM] * len(vmem),
        out_specs=[VMEM] * (len(outs) - scalars) + [SMEM] * scalars,
        scratch_shapes=[pltpu.VMEM(s, F32) for s in scratch],
        compiler_params=pltpu.CompilerParams(vmem_limit_bytes=mib << 20),
        cost_estimate=pl.CostEstimate(flops=flops, bytes_accessed=1 << 20, transcendentals=0),
    )(*smem, *vmem)


def on_device(coef_fine, coef_coarse, rhs_field, level_counts):
    slots, rows, cols = coef_fine.shape
    fields = 2 * slots
    outer, inner = lax.axis_size("slab_0"), lax.axis_size("slab_1")
    levels = lax.axis_size("level")
    slabs = outer * inner
    me = lax.axis_index(SLAB)
    from_above = [(i, i + 1) for i in range(slabs - 1)]
    from_below = [(i + 1, i) for i in range(slabs - 1)]
    here = jnp.concatenate([coef_fine, coef_coarse, rhs_field[None]], axis=0)
    odd_down = [pair for i in range(1, slabs - 1, 2) for pair in ((i, i + 1), (i + 1, i))]
    odd_up = [pair for i in range(0, slabs, 2) for pair in ((i, i + 1), (i + 1, i))]
    one = lax.ppermute(here, SLAB, odd_down)
    two = lax.ppermute(here, SLAB, odd_up)
    edge = jnp.stack([jnp.where(me == 0, 8, 0), jnp.where(me == slabs - 1, 16, 24), me % 2]).astype(jnp.int32)
    place = jnp.stack([me, lax.axis_index("slab_0"), lax.axis_index("level")]).astype(jnp.int32)

    packed, rims, s1, s2, k1, k2, to_below, to_above = call(
        down_kernel,
        [
            shape(inner, LINES, 128),
            shape(slots, 8, cols),
            shape(slots * 16, cols // 2),
            shape(slots * 8, cols // 4),
            shape(slots * 16, cols // 2),
            shape(slots * 8, cols // 4),
            shape(8, cols // 4),
            shape(8, cols // 4),
        ],
        [edge],
        [here, one, two],
        [
            (3, max(cols // 4, 768), 128),
            (3 * fields * cols // 16, 128),
            (3 * fields * cols // 16, 128),
            (fields * 8, 128),
        ],
        20_000_000,
        28,
    )
    lines = lax.all_to_all(packed, "slab_1", 0, 0, tiled=True)
    lines, to_below, to_above = lax.optimization_barrier((lines, to_below, to_above))
    top = lax.ppermute(to_below, SLAB, from_above)
    bottom = lax.ppermute(to_above, SLAB, from_below)
    used = 4 * fields
    wide = jnp.broadcast_to(lines[None, :, :used], (outer, inner, used, 128))
    gathered = lax.all_to_all(wide, "slab_0", 0, 0, tiled=True).reshape(slabs * used, 128)
    e3, message = call(
        functools.partial(coarse_kernel, fields=fields, slabs=slabs, rows=inner, cells=float(rows * slabs * cols)),
        [shape(slots * 8, 256), shape(levels * outer, 1, 128)],
        [place, level_counts],
        [gathered, lines.reshape(inner * LINES, 128), top, bottom],
        [(2, 2 * fields * slabs, 128), (fields * slabs + 16, 256)],
        5_000_000,
        16,
    )
    got = lax.all_to_all(message, ("level", "slab_0"), 0, 0, tiled=True)
    (solutions,) = call(
        up_kernel,
        [shape(slots, rows, cols)],
        [edge],
        [coef_fine, rhs_field, rims, s1, s2, k1, k2, e3, top, bottom],
        [(cols // 2, 128)],
        10_000_000,
        16,
    )
    diffs, moments, estimate = call(
        functools.partial(final_kernel, levels=levels, outer=outer),
        [shape(slots), shape(1, 2), shape(2)],
        [place],
        [got],
        [],
        1_000,
        4,
        3,
    )
    return solutions, diffs, moments, estimate


def solution(mesh):
    slabs = mesh.shape["slab"]
    outer = 4 if slabs >= 64 else 2
    split = Mesh(mesh.devices.reshape(mesh.shape["level"], outer, slabs // outer), ("level", "slab_0", "slab_1"))
    in_specs = (P("level", SLAB, None), P("level", SLAB, None), P(SLAB, None), P("level"))
    out_specs = (P("level", SLAB, None), P("level"), P("level", None), P())
    return jax.shard_map(on_device, mesh=split, in_specs=in_specs, out_specs=out_specs, check_vma=False)
```

```python
import functools

import jax
import jax.numpy as jnp
from jax import lax
from jax.experimental import pallas as pl
from jax.experimental.pallas import tpu as pltpu
from jax.sharding import Mesh
from jax.sharding import PartitionSpec as P

OMEGA = 0.8
SLAB = ("slab_0", "slab_1")
LINES = 40
F32 = jnp.float32


def iota(shape, dim):
    return lax.broadcasted_iota(jnp.int32, shape, dim)


def right_of(x, cols):
    n = x.shape[1]
    y = pltpu.roll(x, n - 1, 1)
    edge = cols - 1 - (n - 128)
    last = jnp.where(iota((x.shape[0], 128), 1) == edge, 0.0, y[:, n - 128 :])
    return last if n == 128 else jnp.concatenate([y[:, : n - 128], last], axis=1)


def first_column(x, edge):
    first = jnp.where(iota((x.shape[0], 128), 1) == 0, edge[:, :128], x[:, :128])
    return first if x.shape[1] == 128 else jnp.concatenate([first, x[:, 128:]], axis=1)


def below(x, period):
    n = x.shape[0]
    shifted = pltpu.roll(x, n - 1, 0)
    if period is None:
        return shifted
    return jnp.where(iota(x.shape, 0) % period == period - 1, 0.0, shifted)


def faces(k, cols, period):
    half = 0.5 * k
    fr = half + right_of(half, cols)
    fl = first_column(pltpu.roll(fr, 1, 1), half)
    fd = half + below(half, period)
    fu = pltpu.roll(fd, 1, 0)
    if period is not None:
        fu = jnp.where(iota(k.shape, 0) % period == 0, half, fu)
    return half, fr, fd, (fr + fl) + (fd + fu)


def across(u, half, fr, cols):
    q = fr * (u - right_of(u, cols))
    return q - first_column(pltpu.roll(q, 1, 1), -half[:, :128] * u[:, :128])


def fluxes(u, half, fr, fd, cols, period):
    p = fd * (u - below(u, period))
    pu = pltpu.roll(p, 1, 0)
    if period is not None:
        pu = jnp.where(iota(u.shape, 0) % period == 0, -half * u, pu)
    return across(u, half, fr, cols) + (p - pu)


def pair_matrix(shape, dim, value):
    long, short = iota(shape, dim), iota(shape, 1 - dim)
    return jnp.where(long // 2 == short, value, 0.0).astype(jnp.bfloat16)


def dot(a, b):
    high = a.astype(jnp.bfloat16)
    rest = a - high.astype(F32)
    middle = rest.astype(jnp.bfloat16)
    low = (rest - middle.astype(F32)).astype(jnp.bfloat16)
    one = functools.partial(jnp.dot, preferred_element_type=F32)
    return one(high, b) + (one(middle, b) + one(low, b))


def pieces(x, width=128):
    return [x[:, i : i + width] for i in range(0, x.shape[1], width)]


def pairs_of_rows(x, scratch):
    rows = x.shape[0]
    room = -(-rows // 16) * 16
    parts = pieces(x)
    for i, piece in enumerate(parts):
        scratch[i * room : i * room + rows, :] = piece
    out = len(parts) * room // 2
    return scratch[pl.ds(0, out, stride=2), :] + scratch[pl.ds(1, out, stride=2), :], room // 2


def halve(x, scratch, quarter):
    tall, rows = pairs_of_rows(x, scratch)
    n = x.shape[1] // 128
    blocks = [tall[i * rows : (i + 1) * rows] for i in range(n)]
    if n == 1:
        return dot(tall, quarter[:128])
    both = jnp.concatenate(
        [jnp.concatenate(blocks[0::2], axis=0), jnp.concatenate(blocks[1::2], axis=0)], axis=1
    )
    got = dot(both, quarter)
    return jnp.concatenate([got[i * rows : (i + 1) * rows] for i in range(n // 2)], axis=1)


def double_cols(x, spread):
    rows = x.shape[0]
    parts = pieces(x)
    got = dot(jnp.concatenate(parts, axis=0), spread)
    return jnp.concatenate([got[i * rows : (i + 1) * rows] for i in range(len(parts))], axis=1)


def double_rows(x, scratch):
    rows = x.shape[0]
    parts = pieces(x)
    for i, piece in enumerate(parts):
        scratch[pl.ds(i * 2 * rows, rows, stride=2), :] = piece
        scratch[pl.ds(i * 2 * rows + 1, rows, stride=2), :] = piece
    return jnp.concatenate([scratch[i * 2 * rows : (i + 1) * 2 * rows, :] for i in range(len(parts))], axis=1)


def inside(shape, depth, edge, window):
    row = iota(shape, 0) % window
    return (row >= (edge[0] >> depth)) & (row < (edge[1] >> depth))


def summed(parts):
    return functools.reduce(jnp.add, parts)


def sweep(k, s, w, depth, window, edge):
    cols = k.shape[1]
    half, fr, fd, diag = faces(k, cols, None)
    scale = jnp.where(inside(k.shape, depth, edge, window), OMEGA / diag, 0.0)
    us = scale * s
    uw = scale if w is None else scale * w
    rs = s - fluxes(us, half, fr, fd, cols, None)
    rw = (1.0 if w is None else w) - fluxes(uw, half, fr, fd, cols, None)
    return us, rs, rw, rw * us + uw * s


def down_kernel(
    edge, here, one, two,
    packed, rims, s1_out, s2_out, k1_out, k2_out, to_below, to_above,
    scratch, even, odd, parts,
):
    quarter = pair_matrix((256, 128), 0, 0.25)
    fields = here.shape[0] - 1
    slots = fields // 2
    copies = packed.shape[0]
    chunks = here.shape[2] // 128
    flip = edge[2] == 1

    def window(at):
        a, b = one[at], two[at]
        return jnp.concatenate([jnp.where(flip, b, a), here[at], jnp.where(flip, a, b)], axis=0)

    source = window(fields)
    for q in range(3):
        for i in range(chunks):
            scratch[q, i * 32 + 24 : i * 32 + 32, :] = jnp.zeros((8, 128), F32)

    def finest(fine, field, _):
        k = window(field)
        us, rs, rw, share = sweep(k, source, None, 0, 24, edge)
        parts[pl.ds(pl.multiple_of(field * 8, 8), 8), :] = summed(pieces(share[8:16]))
        if fine:
            rims[field, 0:1, :] = k[7:8]
            rims[field, 1:2, :] = k[16:17]
            rims[field, 2:3, :] = us[7:8]
            rims[field, 3:4, :] = us[16:17]
        for q, x in enumerate((k, rs, rw)):
            tall, rows = pairs_of_rows(x, scratch.at[q])
            for i in range(chunks):
                into = even if i % 2 == 0 else odd
                at = pl.multiple_of((q * (chunks // 2) + i // 2) * fields * rows + field * rows, 8)
                into[pl.ds(at, rows), :] = tall[i * rows : (i + 1) * rows]
        return 0

    lax.fori_loop(0, slots, functools.partial(finest, True), 0)
    lax.fori_loop(slots, fields, functools.partial(finest, False), 0)

    block = fields * 16
    level = []
    for q in range(3):
        span = slice(q * (chunks // 2) * block, (q + 1) * (chunks // 2) * block)
        got = dot(jnp.concatenate([even[span, :], odd[span, :]], axis=1), quarter)
        level.append(jnp.concatenate([got[i * block : (i + 1) * block] for i in range(chunks // 2)], axis=1))
    for depth, room in ((1, 16), (2, 8)):
        k, s, w = level
        us, rs, rw, share = sweep(k, s, w, depth, room, edge)
        own = 8 >> depth
        row = iota(share.shape, 0) % room
        share = summed(pieces(jnp.where((row >= own) & (row < 2 * own), share, 0.0))) * (16.0**depth)
        for field in range(fields):
            at = field * room
            parts[field * 8 : field * 8 + 8, :] += summed([share[at + i : at + i + 8] for i in range(0, room, 8)])
        kept = slots * room
        if depth == 1:
            s1_out[...], k1_out[...] = s[:kept], k[:kept]
        else:
            s2_out[...], k2_out[...] = s[:kept], k[:kept]
            to_below[...] = jnp.zeros_like(to_below)
            to_above[...] = jnp.zeros_like(to_above)
            for slot in range(slots):
                to_below[slot : slot + 1, :] = us[slot * 8 + 2 : slot * 8 + 3] * 16.0
                to_above[slot : slot + 1, :] = us[slot * 8 + 3 : slot * 8 + 4] * 16.0
        level = [halve(x, scratch.at[q], quarter) for q, x in enumerate((k, rs, rw))]

    for q, x in enumerate(level):
        for field in range(fields):
            for h in range(2):
                line = x[field * 4 + 1 : field * 4 + 2, h * 128 : (h + 1) * 128]
                packed[0, (q * fields + field) * 2 + h : (q * fields + field) * 2 + h + 1, :] = line
    lane = iota((1, 128), 1)
    line = jnp.zeros((1, 128), F32)
    for field in range(fields):
        line = line + jnp.where(lane == field, jnp.sum(parts[field * 8 : field * 8 + 8, :]), 0.0)
    packed[0, 6 * fields : 6 * fields + 1, :] = line
    packed[0, 6 * fields + 1 :, :] = jnp.zeros((LINES - 6 * fields - 1, 128), F32)
    for i in range(1, copies):
        packed[i] = packed[0]


def shared_lines(fields):
    slots = fields // 2
    common = [(q * fields + f) * 2 + h for q in range(2) for f in range(slots) for h in range(2)]
    return common, lambda x: [(q * fields + slots + min(x, slots - 1)) * 2 + h for q in range(3) for h in range(2)]


def fan_kernel(lines, wide, *, fields):
    outer = wide.shape[0]
    common, special = shared_lines(fields)
    rows = wide.shape[1] // (len(common) + 6)
    for at, line in enumerate(common):
        got = lines[pl.ds(line, rows, stride=LINES), :]
        for x in range(outer):
            wide[x, at * rows : (at + 1) * rows, :] = got
    for x in range(outer):
        for at, line in enumerate(special(x)):
            start = (len(common) + at) * rows
            wide[x, start : start + rows, :] = lines[pl.ds(line, rows, stride=LINES), :]


def coarse_kernel(place, counts, gathered, lines, e3, message, scratch, whole, *, fields, slabs, rows, cells):
    slots = fields // 2
    quarter = pair_matrix((256, 128), 0, 0.25)
    spread = pair_matrix((128, 256), 1, 1.0)
    n = slabs
    outer = gathered.shape[0]
    common = 4 * slots

    def taken(at):
        return jnp.concatenate([gathered[x, at * rows : (at + 1) * rows, :] for x in range(outer)], axis=0)

    def field(q, f):
        if f == slots:
            return jnp.concatenate([taken(common + q * 2), taken(common + q * 2 + 1)], axis=1)
        return jnp.concatenate([taken((q * slots + f) * 2), taken((q * slots + f) * 2 + 1)], axis=1)

    k3, s3 = [jnp.concatenate([field(q, f) for f in range(slots + 1)], axis=0) for q in range(2)]
    half3, fr3, fd3, diag3 = faces(k3, 256, n)
    scale3 = OMEGA / diag3
    u3 = scale3 * s3
    k4 = halve(k3, scratch.at[0], quarter)
    s4 = halve(s3 - fluxes(u3, half3, fr3, fd3, 256, n), scratch.at[1], quarter)
    half4, fr4, fd4, diag4 = faces(k4, 128, n // 2)
    scale4 = OMEGA / diag4
    u4 = scale4 * s4
    k5 = halve(k4, scratch.at[0], quarter)
    s5 = halve(s4 - fluxes(u4, half4, fr4, fd4, 128, n // 2), scratch.at[1], quarter)
    half5, fr5, fd5, diag5 = faces(k5, 64, n // 4)
    scale5 = jnp.where(iota(diag5.shape, 1) < 64, OMEGA / diag5, 0.0)
    u5 = scale5 * s5
    for _ in range(3):
        u5 = u5 + scale5 * (s5 - fluxes(u5, half5, fr5, fd5, 64, n // 4))
    u4 = u4 + double_rows(double_cols(u5, spread[:, :128]), scratch.at[0]) * 4.0
    u4 = u4 + scale4 * (s4 - fluxes(u4, half4, fr4, fd4, 128, n // 2))
    u3 = u3 + double_rows(double_cols(u4, spread), scratch.at[0]) * 4.0
    u3 = u3 + scale3 * (s3 - fluxes(u3, half3, fr3, fd3, 256, n))
    v3 = u3 * 64.0
    whole[0:8, :] = jnp.zeros((8, 256), F32)
    whole[8 : 8 + slots * n, :] = v3[: slots * n]
    whole[8 + slots * n :, :] = jnp.zeros((8, 256), F32)

    lane = iota((1, 128), 1)
    block = pl.multiple_of(place[1] * rows, 8)

    def weighed(f):
        v = whole[pl.ds(8 + f * n + block, rows), :]
        w = [lines[pl.ds((2 * fields + f) * 2 + h, rows, stride=LINES), :] for h in range(2)]
        return v[:, :128] * w[0] + v[:, 128:] * w[1]

    total = jnp.sum(lines[pl.ds(6 * fields, rows, stride=LINES), :], axis=0, keepdims=True)
    total = total - pltpu.roll(total, 128 - slots, 1)
    for f in range(slots):
        total = total + jnp.where(lane == f, 64.0 * jnp.sum(weighed(f)), 0.0)
    other = field(2, slots) * v3[slots * n :]
    total = total - jnp.where((lane == place[1]) & (lane < slots), 64.0 * jnp.sum(other), 0.0)
    sent = jnp.where(lane < slots, total / cells, jnp.where(lane == slots, counts[0].astype(F32), 0.0))
    for i in range(message.shape[0]):
        message[i] = sent

    me = place[0]
    e3[...] = jnp.zeros_like(e3)
    for f in range(slots):
        for r in range(3):
            line = whole[pl.ds(8 + f * n + me + (r - 1), 1), :]
            if r == 0:
                line = jnp.where(me > 0, line, 0.0)
            if r == 2:
                line = jnp.where(me < n - 1, line, 0.0)
            e3[f * 8 + r : f * 8 + r + 1, :] = line


def up_kernel(edge, here, g, rims, s1, s2, k1, k2, e3, top, bottom, out, scratch):
    spread = pair_matrix((128, 256), 1, 1.0)
    slots = here.shape[0]

    def relaxed(k, s, e, depth, window, swap):
        half, fr, fd, diag = faces(k, k.shape[1], None)
        scale = OMEGA / diag
        s = s * (4.0**depth)
        valid = inside(k.shape, depth, edge, window)
        v = jnp.where(valid, swap(scale * s) + e, 0.0)
        return jnp.where(valid, v + scale * (s - fluxes(v, half, fr, fd, k.shape[1], None)), 0.0)

    def stacked(ref, rows):
        return jnp.concatenate([jnp.broadcast_to(ref[f : f + 1, :], (rows, ref.shape[1])) for f in range(slots)], axis=0)

    def rimmed(v):
        row = iota(v.shape, 0) % 8
        return jnp.where(row == 0, stacked(top, 8), jnp.where(row == 5, stacked(bottom, 8), v))

    e = double_rows(double_cols(e3[...], spread), scratch)
    e = jnp.concatenate([e[f * 16 : f * 16 + 8] for f in range(slots)], axis=0)
    e = relaxed(k2[...], s2[...], e, 2, 8, rimmed)
    e = double_rows(double_cols(e, spread), scratch)
    e = relaxed(k1[...], s1[...], e, 1, 16, lambda v: v)
    e = double_cols(e, spread)
    g = g[...]
    row = iota(g.shape, 0)
    cols = g.shape[1]

    def lower(x, last):
        return jnp.where(row == 7, last, pltpu.roll(x, 7, 0))

    def upper(x, first):
        return jnp.where(row == 0, first, pltpu.roll(x, 1, 0))

    for f in range(slots):
        k = here[f]
        half = 0.5 * k
        fr = half + right_of(half, cols)
        fl = first_column(pltpu.roll(fr, 1, 1), half)
        fd = half + lower(half, 0.5 * rims[f, 1:2, :])
        fu = half + upper(half, 0.5 * rims[f, 0:1, :])
        scale = OMEGA / ((fr + fl) + (fd + fu))
        at = f * 16
        v = scale * g + double_rows(e[at : at + 8], scratch)[8:16]
        first = rims[f, 2:3, :] + e[at + 3 : at + 4]
        last = rims[f, 3:4, :] + e[at + 8 : at + 9]
        flow = across(v, half, fr, cols) + (fd * (v - lower(v, last)) + fu * (v - upper(v, first)))
        out[f] = v + scale * (g - flow)


def final_kernel(place, got, diffs, moments, estimate, *, levels, outer):
    slots = diffs.shape[0]
    row, lane = iota((8, 128), 0), iota((8, 128), 1)
    table = jnp.zeros((8, 128), F32)
    for m in range(levels):
        table = jnp.where(row == m, summed([got[m * outer + i] for i in range(outer)]), table)

    def along(x):
        return jnp.sum(x, axis=1, keepdims=True)

    counted = along(jnp.where(lane == slots, table, 0.0)) / outer
    counted = jnp.where(row[:, :1] < levels, counted, 1.0)
    live = (lane < slots) & (lane.astype(F32) < counted) & (row < levels)
    mean = along(jnp.where(live, table, 0.0)) / counted
    spare = jnp.where(live, table - mean, 0.0)
    var = along(spare * spare) / jnp.maximum(counted - 1.0, 1.0)
    both = jnp.where(lane == 0, mean, jnp.where(lane == 1, var, 0.0))
    sums = jnp.where(lane == 0, mean, jnp.where(lane == 1, var / counted, 0.0))
    sums = jnp.sum(sums, axis=0, keepdims=True)
    mine = row == place[2]
    own = jnp.sum(jnp.where(mine, table, 0.0), axis=0, keepdims=True)
    both = jnp.sum(jnp.where(mine, both, 0.0), axis=0, keepdims=True)
    for i in range(slots):
        diffs[i] = own[0, i]
    for i in range(2):
        moments[0, i] = both[0, i]
        estimate[i] = sums[0, i]


VMEM = pl.BlockSpec(memory_space=pltpu.VMEM)
SMEM = pl.BlockSpec(memory_space=pltpu.SMEM)


def shape(*dims):
    return jax.ShapeDtypeStruct(dims, F32)


def call(kernel, outs, smem, vmem, scratch, flops, mib, scalars=0):
    return pl.pallas_call(
        kernel,
        out_shape=outs,
        in_specs=[SMEM] * len(smem) + [VMEM] * len(vmem),
        out_specs=[VMEM] * (len(outs) - scalars) + [SMEM] * scalars,
        scratch_shapes=[pltpu.VMEM(s, F32) for s in scratch],
        compiler_params=pltpu.CompilerParams(vmem_limit_bytes=mib << 20),
        cost_estimate=pl.CostEstimate(flops=flops, bytes_accessed=1 << 20, transcendentals=0),
    )(*smem, *vmem)


def on_device(coef_fine, coef_coarse, rhs_field, level_counts):
    slots, rows, cols = coef_fine.shape
    fields = 2 * slots
    outer, inner = lax.axis_size("slab_0"), lax.axis_size("slab_1")
    levels = lax.axis_size("level")
    slabs = outer * inner
    me = lax.axis_index(SLAB)
    from_above = [(i, i + 1) for i in range(slabs - 1)]
    from_below = [(i + 1, i) for i in range(slabs - 1)]
    here = jnp.concatenate([coef_fine, coef_coarse, rhs_field[None]], axis=0)
    odd_down = [pair for i in range(1, slabs - 1, 2) for pair in ((i, i + 1), (i + 1, i))]
    odd_up = [pair for i in range(0, slabs, 2) for pair in ((i, i + 1), (i + 1, i))]
    one = lax.ppermute(here, SLAB, odd_down)
    two = lax.ppermute(here, SLAB, odd_up)
    edge = jnp.stack([jnp.where(me == 0, 8, 0), jnp.where(me == slabs - 1, 16, 24), me % 2]).astype(jnp.int32)
    place = jnp.stack([me, lax.axis_index("slab_0"), lax.axis_index("level")]).astype(jnp.int32)

    packed, rims, s1, s2, k1, k2, to_below, to_above = call(
        down_kernel,
        [
            shape(inner, LINES, 128),
            shape(slots, 8, cols),
            shape(slots * 16, cols // 2),
            shape(slots * 8, cols // 4),
            shape(slots * 16, cols // 2),
            shape(slots * 8, cols // 4),
            shape(8, cols // 4),
            shape(8, cols // 4),
        ],
        [edge],
        [here, one, two],
        [
            (3, max(cols // 4, 768), 128),
            (3 * fields * cols // 16, 128),
            (3 * fields * cols // 16, 128),
            (fields * 8, 128),
        ],
        20_000_000,
        28,
    )
    lines = lax.all_to_all(packed, "slab_1", 0, 0, tiled=True)
    top = lax.ppermute(to_below, SLAB, from_above)
    bottom = lax.ppermute(to_above, SLAB, from_below)
    lines, top, bottom = lax.optimization_barrier((lines, top, bottom))
    lines = lines.reshape(inner * LINES, 128)
    (wide,) = call(
        functools.partial(fan_kernel, fields=fields),
        [shape(outer, (4 * slots + 6) * inner, 128)],
        [],
        [lines],
        [],
        1_000_000,
        8,
    )
    gathered = lax.all_to_all(wide, "slab_0", 0, 0, tiled=True)
    e3, message = call(
        functools.partial(coarse_kernel, fields=fields, slabs=slabs, rows=inner, cells=float(rows * slabs * cols)),
        [shape(slots * 8, 256), shape(levels * outer, 1, 128)],
        [place, level_counts],
        [gathered, lines],
        [(2, 2 * (slots + 1) * slabs, 128), (slots * slabs + 16, 256)],
        5_000_000,
        16,
    )
    got = lax.all_to_all(message, ("level", "slab_0"), 0, 0, tiled=True)
    (solutions,) = call(
        up_kernel,
        [shape(slots, rows, cols)],
        [edge],
        [coef_fine, rhs_field, rims, s1, s2, k1, k2, e3, top, bottom],
        [(cols // 2, 128)],
        10_000_000,
        16,
    )
    diffs, moments, estimate = call(
        functools.partial(final_kernel, levels=levels, outer=outer),
        [shape(slots), shape(1, 2), shape(2)],
        [place],
        [got],
        [],
        1_000,
        4,
        3,
    )
    return solutions, diffs, moments, estimate


def solution(mesh):
    slabs = mesh.shape["slab"]
    outer = 4 if slabs >= 64 else 2
    split = Mesh(mesh.devices.reshape(mesh.shape["level"], outer, slabs // outer), ("level", "slab_0", "slab_1"))
    in_specs = (P("level", SLAB, None), P("level", SLAB, None), P(SLAB, None), P("level"))
    out_specs = (P("level", SLAB, None), P("level"), P("level", None), P())
    return jax.shard_map(on_device, mesh=split, in_specs=in_specs, out_specs=out_specs, check_vma=False)
```

```python
import functools

import jax
import jax.numpy as jnp
from jax import lax
from jax.experimental import pallas as pl
from jax.experimental.pallas import tpu as pltpu
from jax.sharding import Mesh
from jax.sharding import PartitionSpec as P

OMEGA = 0.8
SLAB = ("slab_0", "slab_1")
LINES = 40
F32 = jnp.float32


def iota(shape, dim):
    return lax.broadcasted_iota(jnp.int32, shape, dim)


def right_of(x, cols):
    n = x.shape[1]
    y = pltpu.roll(x, n - 1, 1)
    edge = cols - 1 - (n - 128)
    last = jnp.where(iota((x.shape[0], 128), 1) == edge, 0.0, y[:, n - 128 :])
    return last if n == 128 else jnp.concatenate([y[:, : n - 128], last], axis=1)


def first_column(x, edge):
    first = jnp.where(iota((x.shape[0], 128), 1) == 0, edge[:, :128], x[:, :128])
    return first if x.shape[1] == 128 else jnp.concatenate([first, x[:, 128:]], axis=1)


def below(x, period):
    n = x.shape[0]
    shifted = pltpu.roll(x, n - 1, 0)
    if period is None:
        return shifted
    return jnp.where(iota(x.shape, 0) % period == period - 1, 0.0, shifted)


def faces(k, cols, period):
    half = 0.5 * k
    fr = half + right_of(half, cols)
    fl = first_column(pltpu.roll(fr, 1, 1), half)
    fd = half + below(half, period)
    fu = pltpu.roll(fd, 1, 0)
    if period is not None:
        fu = jnp.where(iota(k.shape, 0) % period == 0, half, fu)
    return half, fr, fd, (fr + fl) + (fd + fu)


def across(u, half, fr, cols):
    q = fr * (u - right_of(u, cols))
    return q - first_column(pltpu.roll(q, 1, 1), -half[:, :128] * u[:, :128])


def fluxes(u, half, fr, fd, cols, period):
    p = fd * (u - below(u, period))
    pu = pltpu.roll(p, 1, 0)
    if period is not None:
        pu = jnp.where(iota(u.shape, 0) % period == 0, -half * u, pu)
    return across(u, half, fr, cols) + (p - pu)


def pair_matrix(shape, dim, value):
    long, short = iota(shape, dim), iota(shape, 1 - dim)
    return jnp.where(long // 2 == short, value, 0.0).astype(jnp.bfloat16)


def dot(a, b):
    high = a.astype(jnp.bfloat16)
    rest = a - high.astype(F32)
    middle = rest.astype(jnp.bfloat16)
    low = (rest - middle.astype(F32)).astype(jnp.bfloat16)
    one = functools.partial(jnp.dot, preferred_element_type=F32)
    return one(high, b) + (one(middle, b) + one(low, b))


def pieces(x, width=128):
    return [x[:, i : i + width] for i in range(0, x.shape[1], width)]


def pairs_of_rows(x, scratch):
    rows = x.shape[0]
    room = -(-rows // 16) * 16
    parts = pieces(x)
    for i, piece in enumerate(parts):
        scratch[i * room : i * room + rows, :] = piece
    out = len(parts) * room // 2
    return scratch[pl.ds(0, out, stride=2), :] + scratch[pl.ds(1, out, stride=2), :], room // 2


def halve(x, scratch, quarter):
    tall, rows = pairs_of_rows(x, scratch)
    n = x.shape[1] // 128
    blocks = [tall[i * rows : (i + 1) * rows] for i in range(n)]
    if n == 1:
        return dot(tall, quarter[:128])
    both = jnp.concatenate(
        [jnp.concatenate(blocks[0::2], axis=0), jnp.concatenate(blocks[1::2], axis=0)], axis=1
    )
    got = dot(both, quarter)
    return jnp.concatenate([got[i * rows : (i + 1) * rows] for i in range(n // 2)], axis=1)


def double_cols(x, spread):
    rows = x.shape[0]
    parts = pieces(x)
    got = dot(jnp.concatenate(parts, axis=0), spread)
    return jnp.concatenate([got[i * rows : (i + 1) * rows] for i in range(len(parts))], axis=1)


def double_rows(x, scratch):
    rows = x.shape[0]
    parts = pieces(x)
    for i, piece in enumerate(parts):
        scratch[pl.ds(i * 2 * rows, rows, stride=2), :] = piece
        scratch[pl.ds(i * 2 * rows + 1, rows, stride=2), :] = piece
    return jnp.concatenate([scratch[i * 2 * rows : (i + 1) * 2 * rows, :] for i in range(len(parts))], axis=1)


def inside(shape, depth, edge, window):
    row = iota(shape, 0) % window
    return (row >= (edge[0] >> depth)) & (row < (edge[1] >> depth))


def summed(parts):
    return functools.reduce(jnp.add, parts)


def sweep(k, s, w, depth, window, edge):
    cols = k.shape[1]
    half, fr, fd, diag = faces(k, cols, None)
    scale = jnp.where(inside(k.shape, depth, edge, window), OMEGA / diag, 0.0)
    us = scale * s
    uw = scale if w is None else scale * w
    rs = s - fluxes(us, half, fr, fd, cols, None)
    rw = (1.0 if w is None else w) - fluxes(uw, half, fr, fd, cols, None)
    return us, rs, rw, rw * us + uw * s


def down_kernel(
    edge, here, one, two,
    packed, rims, s1_out, s2_out, k1_out, k2_out, to_far, to_near,
    scratch, even, odd, parts,
):
    quarter = pair_matrix((256, 128), 0, 0.25)
    fields = here.shape[0] - 1
    slots = fields // 2
    copies = packed.shape[0]
    chunks = here.shape[2] // 128
    flip = edge[2] == 1

    def window(at):
        a, b = one[at], two[at]
        return jnp.concatenate([jnp.where(flip, b, a), here[at], jnp.where(flip, a, b)], axis=0)

    source = window(fields)
    for q in range(3):
        for i in range(chunks):
            scratch[q, i * 32 + 24 : i * 32 + 32, :] = jnp.zeros((8, 128), F32)

    def finest(fine, field, _):
        k = window(field)
        us, rs, rw, share = sweep(k, source, None, 0, 24, edge)
        parts[pl.ds(pl.multiple_of(field * 8, 8), 8), :] = summed(pieces(share[8:16]))
        if fine:
            rims[field, 0:1, :] = k[7:8]
            rims[field, 1:2, :] = k[16:17]
            rims[field, 2:3, :] = us[7:8]
            rims[field, 3:4, :] = us[16:17]
        for q, x in enumerate((k, rs, rw)):
            tall, rows = pairs_of_rows(x, scratch.at[q])
            for i in range(chunks):
                into = even if i % 2 == 0 else odd
                at = pl.multiple_of((q * (chunks // 2) + i // 2) * fields * rows + field * rows, 8)
                into[pl.ds(at, rows), :] = tall[i * rows : (i + 1) * rows]
        return 0

    lax.fori_loop(0, slots, functools.partial(finest, True), 0)
    lax.fori_loop(slots, fields, functools.partial(finest, False), 0)

    block = fields * 16
    level = []
    for q in range(3):
        span = slice(q * (chunks // 2) * block, (q + 1) * (chunks // 2) * block)
        got = dot(jnp.concatenate([even[span, :], odd[span, :]], axis=1), quarter)
        level.append(jnp.concatenate([got[i * block : (i + 1) * block] for i in range(chunks // 2)], axis=1))
    for depth, room in ((1, 16), (2, 8)):
        k, s, w = level
        us, rs, rw, share = sweep(k, s, w, depth, room, edge)
        own = 8 >> depth
        row = iota(share.shape, 0) % room
        share = summed(pieces(jnp.where((row >= own) & (row < 2 * own), share, 0.0))) * (16.0**depth)
        for field in range(fields):
            at = field * room
            parts[field * 8 : field * 8 + 8, :] += summed([share[at + i : at + i + 8] for i in range(0, room, 8)])
        kept = slots * room
        if depth == 1:
            s1_out[...], k1_out[...] = s[:kept], k[:kept]
        else:
            s2_out[...], k2_out[...] = s[:kept], k[:kept]
            to_far[...] = jnp.zeros_like(to_far)
            to_near[...] = jnp.zeros_like(to_near)
            for slot in range(slots):
                upper, lower = us[slot * 8 + 2 : slot * 8 + 3] * 16.0, us[slot * 8 + 3 : slot * 8 + 4] * 16.0
                to_far[slot : slot + 1, :] = jnp.where(flip, upper, lower)
                to_near[slot : slot + 1, :] = jnp.where(flip, lower, upper)
        level = [halve(x, scratch.at[q], quarter) for q, x in enumerate((k, rs, rw))]

    for q, x in enumerate(level):
        for field in range(fields):
            for h in range(2):
                line = x[field * 4 + 1 : field * 4 + 2, h * 128 : (h + 1) * 128]
                packed[0, (q * fields + field) * 2 + h : (q * fields + field) * 2 + h + 1, :] = line
    lane = iota((1, 128), 1)
    line = jnp.zeros((1, 128), F32)
    for field in range(fields):
        line = line + jnp.where(lane == field, jnp.sum(parts[field * 8 : field * 8 + 8, :]), 0.0)
    packed[0, 6 * fields : 6 * fields + 1, :] = line
    packed[0, 6 * fields + 1 :, :] = jnp.zeros((LINES - 6 * fields - 1, 128), F32)
    for i in range(1, copies):
        packed[i] = packed[0]


def shared_lines(fields):
    slots = fields // 2
    common = [(q * fields + f) * 2 + h for q in range(2) for f in range(slots) for h in range(2)]
    return common, lambda x: [(q * fields + slots + min(x, slots - 1)) * 2 + h for q in range(3) for h in range(2)]


def fan_kernel(lines, wide, *, fields):
    outer = wide.shape[0]
    common, special = shared_lines(fields)
    rows = wide.shape[1] // (len(common) + 6)
    for at, line in enumerate(common):
        got = lines[pl.ds(line, rows, stride=LINES), :]
        for x in range(outer):
            wide[x, at * rows : (at + 1) * rows, :] = got
    for x in range(outer):
        for at, line in enumerate(special(x)):
            start = (len(common) + at) * rows
            wide[x, start : start + rows, :] = lines[pl.ds(line, rows, stride=LINES), :]


def coarse_kernel(place, gathered, lines, e3, message, scratch, whole, *, fields, slabs, rows, cells):
    slots = fields // 2
    quarter = pair_matrix((256, 128), 0, 0.25)
    spread = pair_matrix((128, 256), 1, 1.0)
    n = slabs
    outer = gathered.shape[0]
    common = 4 * slots

    def taken(at):
        return jnp.concatenate([gathered[x, at * rows : (at + 1) * rows, :] for x in range(outer)], axis=0)

    def field(q, f):
        if f == slots:
            return jnp.concatenate([taken(common + q * 2), taken(common + q * 2 + 1)], axis=1)
        return jnp.concatenate([taken((q * slots + f) * 2), taken((q * slots + f) * 2 + 1)], axis=1)

    k3, s3 = [jnp.concatenate([field(q, f) for f in range(slots + 1)], axis=0) for q in range(2)]
    half3, fr3, fd3, diag3 = faces(k3, 256, n)
    scale3 = OMEGA / diag3
    u3 = scale3 * s3
    k4 = halve(k3, scratch.at[0], quarter)
    s4 = halve(s3 - fluxes(u3, half3, fr3, fd3, 256, n), scratch.at[1], quarter)
    half4, fr4, fd4, diag4 = faces(k4, 128, n // 2)
    scale4 = OMEGA / diag4
    u4 = scale4 * s4
    k5 = halve(k4, scratch.at[0], quarter)
    s5 = halve(s4 - fluxes(u4, half4, fr4, fd4, 128, n // 2), scratch.at[1], quarter)
    half5, fr5, fd5, diag5 = faces(k5, 64, n // 4)
    scale5 = jnp.where(iota(diag5.shape, 1) < 64, OMEGA / diag5, 0.0)
    u5 = scale5 * s5
    for _ in range(3):
        u5 = u5 + scale5 * (s5 - fluxes(u5, half5, fr5, fd5, 64, n // 4))
    u4 = u4 + double_rows(double_cols(u5, spread[:, :128]), scratch.at[0]) * 4.0
    u4 = u4 + scale4 * (s4 - fluxes(u4, half4, fr4, fd4, 128, n // 2))
    u3 = u3 + double_rows(double_cols(u4, spread), scratch.at[0]) * 4.0
    u3 = u3 + scale3 * (s3 - fluxes(u3, half3, fr3, fd3, 256, n))
    v3 = u3 * 64.0
    whole[0:8, :] = jnp.zeros((8, 256), F32)
    whole[8 : 8 + slots * n, :] = v3[: slots * n]
    whole[8 + slots * n :, :] = jnp.zeros((8, 256), F32)

    lane = iota((1, 128), 1)
    block = pl.multiple_of(place[5] * rows, 8)

    def weighed(f):
        v = whole[pl.ds(8 + f * n + block, rows), :]
        w = [lines[pl.ds((2 * fields + f) * 2 + h, rows, stride=LINES), :] for h in range(2)]
        return v[:, :128] * w[0] + v[:, 128:] * w[1]

    total = jnp.sum(lines[pl.ds(6 * fields, rows, stride=LINES), :], axis=0, keepdims=True)
    total = total - pltpu.roll(total, 128 - slots, 1)
    for f in range(slots):
        total = total + jnp.where(lane == f, 64.0 * jnp.sum(weighed(f)), 0.0)
    other = field(2, slots) * v3[slots * n :]
    total = total - jnp.where((lane == place[5]) & (lane < slots), 64.0 * jnp.sum(other), 0.0)
    sent = jnp.where(lane < slots, total / cells, jnp.where(lane == slots, place[7].astype(F32), 0.0))
    for i in range(message.shape[0]):
        message[i] = sent

    me = place[4]
    e3[...] = jnp.zeros_like(e3)
    for f in range(slots):
        for r in range(3):
            line = whole[pl.ds(8 + f * n + me + (r - 1), 1), :]
            if r == 0:
                line = jnp.where(me > 0, line, 0.0)
            if r == 2:
                line = jnp.where(me < n - 1, line, 0.0)
            e3[f * 8 + r : f * 8 + r + 1, :] = line


def up_kernel(edge, here, rims, s1, s2, k1, k2, e3, far, near, out, scratch):
    spread = pair_matrix((128, 256), 1, 1.0)
    slots = out.shape[0]

    def relaxed(k, s, e, depth, window, swap):
        half, fr, fd, diag = faces(k, k.shape[1], None)
        scale = OMEGA / diag
        s = s * (4.0**depth)
        valid = inside(k.shape, depth, edge, window)
        v = jnp.where(valid, swap(scale * s) + e, 0.0)
        return jnp.where(valid, v + scale * (s - fluxes(v, half, fr, fd, k.shape[1], None)), 0.0)

    def stacked(ref, rows):
        return jnp.concatenate([jnp.broadcast_to(ref[f : f + 1, :], (rows, ref.shape[1])) for f in range(slots)], axis=0)

    def rimmed(v):
        row = iota(v.shape, 0) % 8
        flip = edge[2] == 1
        a, b = stacked(far, 8), stacked(near, 8)
        return jnp.where(row == 0, jnp.where(flip, b, a), jnp.where(row == 5, jnp.where(flip, a, b), v))

    e = double_rows(double_cols(e3[...], spread), scratch)
    e = jnp.concatenate([e[f * 16 : f * 16 + 8] for f in range(slots)], axis=0)
    e = relaxed(k2[...], s2[...], e, 2, 8, rimmed)
    e = double_rows(double_cols(e, spread), scratch)
    e = relaxed(k1[...], s1[...], e, 1, 16, lambda v: v)
    e = double_cols(e, spread)
    g = here[2 * slots]
    row = iota(g.shape, 0)
    cols = g.shape[1]

    def lower(x, last):
        return jnp.where(row == 7, last, pltpu.roll(x, 7, 0))

    def upper(x, first):
        return jnp.where(row == 0, first, pltpu.roll(x, 1, 0))

    for f in range(slots):
        k = here[f]
        half = 0.5 * k
        fr = half + right_of(half, cols)
        fl = first_column(pltpu.roll(fr, 1, 1), half)
        fd = half + lower(half, 0.5 * rims[f, 1:2, :])
        fu = half + upper(half, 0.5 * rims[f, 0:1, :])
        scale = OMEGA / ((fr + fl) + (fd + fu))
        at = f * 16
        v = scale * g + double_rows(e[at : at + 8], scratch)[8:16]
        first = rims[f, 2:3, :] + e[at + 3 : at + 4]
        last = rims[f, 3:4, :] + e[at + 8 : at + 9]
        flow = across(v, half, fr, cols) + (fd * (v - lower(v, last)) + fu * (v - upper(v, first)))
        out[f] = v + scale * (g - flow)


def final_kernel(place, got, diffs, moments, estimate, *, levels, outer):
    slots = diffs.shape[0]
    row, lane = iota((8, 128), 0), iota((8, 128), 1)
    table = jnp.zeros((8, 128), F32)
    for m in range(levels):
        table = jnp.where(row == m, summed([got[m * outer + i] for i in range(outer)]), table)

    def along(x):
        return jnp.sum(x, axis=1, keepdims=True)

    counted = along(jnp.where(lane == slots, table, 0.0)) / outer
    counted = jnp.where(row[:, :1] < levels, counted, 1.0)
    live = (lane < slots) & (lane.astype(F32) < counted) & (row < levels)
    mean = along(jnp.where(live, table, 0.0)) / counted
    spare = jnp.where(live, table - mean, 0.0)
    var = along(spare * spare) / jnp.maximum(counted - 1.0, 1.0)
    both = jnp.where(lane == 0, mean, jnp.where(lane == 1, var, 0.0))
    sums = jnp.where(lane == 0, mean, jnp.where(lane == 1, var / counted, 0.0))
    sums = jnp.sum(sums, axis=0, keepdims=True)
    mine = row == place[6]
    own = jnp.sum(jnp.where(mine, table, 0.0), axis=0, keepdims=True)
    both = jnp.sum(jnp.where(mine, both, 0.0), axis=0, keepdims=True)
    for i in range(slots):
        diffs[i] = own[0, i]
    for i in range(2):
        moments[0, i] = both[0, i]
        estimate[i] = sums[0, i]


VMEM = pl.BlockSpec(memory_space=pltpu.VMEM)
SMEM = pl.BlockSpec(memory_space=pltpu.SMEM)


def shape(*dims):
    return jax.ShapeDtypeStruct(dims, F32)


def call(kernel, outs, smem, vmem, scratch, flops, mib, scalars=0):
    return pl.pallas_call(
        kernel,
        out_shape=outs,
        in_specs=[SMEM] * len(smem) + [VMEM] * len(vmem),
        out_specs=[VMEM] * (len(outs) - scalars) + [SMEM] * scalars,
        scratch_shapes=[pltpu.VMEM(s, F32) for s in scratch],
        compiler_params=pltpu.CompilerParams(vmem_limit_bytes=mib << 20),
        cost_estimate=pl.CostEstimate(flops=flops, bytes_accessed=1 << 20, transcendentals=0),
    )(*smem, *vmem)


def on_device(coef_fine, coef_coarse, rhs_field, level_counts):
    slots, rows, cols = coef_fine.shape
    fields = 2 * slots
    outer, inner = lax.axis_size("slab_0"), lax.axis_size("slab_1")
    levels = lax.axis_size("level")
    slabs = outer * inner
    me = lax.axis_index(SLAB)
    here = jnp.concatenate([coef_fine, coef_coarse, rhs_field[None]], axis=0)
    odd_down = [pair for i in range(1, slabs - 1, 2) for pair in ((i, i + 1), (i + 1, i))]
    odd_up = [pair for i in range(0, slabs, 2) for pair in ((i, i + 1), (i + 1, i))]
    one = lax.ppermute(here, SLAB, odd_down)
    two = lax.ppermute(here, SLAB, odd_up)
    x, z, level = [lax.axis_index(axis) for axis in ("slab_0", "slab_1", "level")]
    spot = [jnp.where(me == 0, 8, 0), jnp.where(me == slabs - 1, 16, 24), me % 2, z, me, x, level, level_counts[0]]
    edge = jnp.stack([jnp.asarray(value, jnp.int32) for value in spot])

    packed, rims, s1, s2, k1, k2, to_far, to_near = call(
        down_kernel,
        [
            shape(inner, LINES, 128),
            shape(slots, 8, cols),
            shape(slots * 16, cols // 2),
            shape(slots * 8, cols // 4),
            shape(slots * 16, cols // 2),
            shape(slots * 8, cols // 4),
            shape(8, cols // 4),
            shape(8, cols // 4),
        ],
        [edge],
        [here, one, two],
        [
            (3, max(cols // 4, 768), 128),
            (3 * fields * cols // 16, 128),
            (3 * fields * cols // 16, 128),
            (fields * 8, 128),
        ],
        20_000_000,
        28,
    )
    lines = lax.all_to_all(packed, "slab_1", 0, 0, tiled=True)
    far = lax.ppermute(to_far, SLAB, odd_down)
    near = lax.ppermute(to_near, SLAB, odd_up)
    lines, far, near = lax.optimization_barrier((lines, far, near))
    lines = lines.reshape(inner * LINES, 128)
    (wide,) = call(
        functools.partial(fan_kernel, fields=fields),
        [shape(outer, (4 * slots + 6) * inner, 128)],
        [],
        [lines],
        [],
        1_000_000,
        8,
    )
    gathered = lax.all_to_all(wide, "slab_0", 0, 0, tiled=True)
    e3, message = call(
        functools.partial(coarse_kernel, fields=fields, slabs=slabs, rows=inner, cells=float(rows * slabs * cols)),
        [shape(slots * 8, 256), shape(levels * outer, 1, 128)],
        [edge],
        [gathered, lines],
        [(2, 2 * (slots + 1) * slabs, 128), (slots * slabs + 16, 256)],
        5_000_000,
        16,
    )
    got = lax.all_to_all(message, ("level", "slab_0"), 0, 0, tiled=True)
    (solutions,) = call(
        up_kernel,
        [shape(slots, rows, cols)],
        [edge],
        [here, rims, s1, s2, k1, k2, e3, far, near],
        [(cols // 2, 128)],
        10_000_000,
        16,
    )
    diffs, moments, estimate = call(
        functools.partial(final_kernel, levels=levels, outer=outer),
        [shape(slots), shape(1, 2), shape(2)],
        [edge],
        [got],
        [],
        1_000,
        4,
        3,
    )
    return solutions, diffs, moments, estimate


def solution(mesh):
    slabs = mesh.shape["slab"]
    outer = 4 if slabs >= 64 else 2
    split = Mesh(mesh.devices.reshape(mesh.shape["level"], outer, slabs // outer), ("level", "slab_0", "slab_1"))
    in_specs = (P("level", SLAB, None), P("level", SLAB, None), P(SLAB, None), P("level"))
    out_specs = (P("level", SLAB, None), P("level"), P("level", None), P())
    return jax.shard_map(on_device, mesh=split, in_specs=in_specs, out_specs=out_specs, check_vma=False)
```

```python
import functools

import jax
import jax.numpy as jnp
from jax import lax
from jax.experimental import pallas as pl
from jax.experimental.pallas import tpu as pltpu
from jax.sharding import Mesh
from jax.sharding import PartitionSpec as P

OMEGA = 0.8
SLAB = ("slab_0", "slab_1")
LINES = 40
F32 = jnp.float32


def iota(shape, dim):
    return lax.broadcasted_iota(jnp.int32, shape, dim)


def right_of(x, cols):
    n = x.shape[1]
    y = pltpu.roll(x, n - 1, 1)
    edge = cols - 1 - (n - 128)
    last = jnp.where(iota((x.shape[0], 128), 1) == edge, 0.0, y[:, n - 128 :])
    return last if n == 128 else jnp.concatenate([y[:, : n - 128], last], axis=1)


def first_column(x, edge):
    first = jnp.where(iota((x.shape[0], 128), 1) == 0, edge[:, :128], x[:, :128])
    return first if x.shape[1] == 128 else jnp.concatenate([first, x[:, 128:]], axis=1)


def below(x, period):
    n = x.shape[0]
    shifted = pltpu.roll(x, n - 1, 0)
    if period is None:
        return shifted
    return jnp.where(iota(x.shape, 0) % period == period - 1, 0.0, shifted)


def faces(k, cols, period):
    half = 0.5 * k
    fr = half + right_of(half, cols)
    fl = first_column(pltpu.roll(fr, 1, 1), half)
    fd = half + below(half, period)
    fu = pltpu.roll(fd, 1, 0)
    if period is not None:
        fu = jnp.where(iota(k.shape, 0) % period == 0, half, fu)
    return half, fr, fd, (fr + fl) + (fd + fu)


def across(u, half, fr, cols):
    q = fr * (u - right_of(u, cols))
    return q - first_column(pltpu.roll(q, 1, 1), -half[:, :128] * u[:, :128])


def fluxes(u, half, fr, fd, cols, period):
    p = fd * (u - below(u, period))
    pu = pltpu.roll(p, 1, 0)
    if period is not None:
        pu = jnp.where(iota(u.shape, 0) % period == 0, -half * u, pu)
    return across(u, half, fr, cols) + (p - pu)


def pair_matrix(shape, dim, value):
    long, short = iota(shape, dim), iota(shape, 1 - dim)
    return jnp.where(long // 2 == short, value, 0.0).astype(jnp.bfloat16)


def dot(a, b):
    high = a.astype(jnp.bfloat16)
    rest = a - high.astype(F32)
    middle = rest.astype(jnp.bfloat16)
    low = (rest - middle.astype(F32)).astype(jnp.bfloat16)
    rows = a.shape[0]
    got = jnp.dot(jnp.concatenate([high, middle, low], axis=0), b, preferred_element_type=F32)
    return got[:rows] + (got[rows : 2 * rows] + got[2 * rows :])


def pieces(x, width=128):
    return [x[:, i : i + width] for i in range(0, x.shape[1], width)]


def pairs_of_rows(x, scratch):
    rows = x.shape[0]
    room = -(-rows // 16) * 16
    parts = pieces(x)
    for i, piece in enumerate(parts):
        scratch[i * room : i * room + rows, :] = piece
    out = len(parts) * room // 2
    return scratch[pl.ds(0, out, stride=2), :] + scratch[pl.ds(1, out, stride=2), :], room // 2


def halve(x, scratch, quarter):
    tall, rows = pairs_of_rows(x, scratch)
    n = x.shape[1] // 128
    blocks = [tall[i * rows : (i + 1) * rows] for i in range(n)]
    if n == 1:
        return dot(tall, quarter[:128])
    both = jnp.concatenate(
        [jnp.concatenate(blocks[0::2], axis=0), jnp.concatenate(blocks[1::2], axis=0)], axis=1
    )
    got = dot(both, quarter)
    return jnp.concatenate([got[i * rows : (i + 1) * rows] for i in range(n // 2)], axis=1)


def double_cols(x, spread):
    rows = x.shape[0]
    parts = pieces(x)
    got = dot(jnp.concatenate(parts, axis=0), spread)
    return jnp.concatenate([got[i * rows : (i + 1) * rows] for i in range(len(parts))], axis=1)


def double_rows(x, scratch):
    rows = x.shape[0]
    parts = pieces(x)
    for i, piece in enumerate(parts):
        scratch[pl.ds(i * 2 * rows, rows, stride=2), :] = piece
        scratch[pl.ds(i * 2 * rows + 1, rows, stride=2), :] = piece
    return jnp.concatenate([scratch[i * 2 * rows : (i + 1) * 2 * rows, :] for i in range(len(parts))], axis=1)


def inside(shape, depth, edge, window):
    row = iota(shape, 0) % window
    return (row >= (edge[0] >> depth)) & (row < (edge[1] >> depth))


def summed(parts):
    return functools.reduce(jnp.add, parts)


def sweep(k, s, w, depth, window, edge):
    cols = k.shape[1]
    half, fr, fd, diag = faces(k, cols, None)
    scale = jnp.where(inside(k.shape, depth, edge, window), OMEGA / diag, 0.0)
    us = scale * s
    uw = scale if w is None else scale * w
    rs = s - fluxes(us, half, fr, fd, cols, None)
    rw = (1.0 if w is None else w) - fluxes(uw, half, fr, fd, cols, None)
    return us, rs, rw, rw * us + uw * s


def down_kernel(
    edge, here, one, two,
    packed, rims, s1_out, s2_out, k1_out, k2_out, to_far, to_near,
    scratch, even, odd, parts,
):
    quarter = pair_matrix((256, 128), 0, 0.25)
    fields = here.shape[0] - 1
    slots = fields // 2
    copies = packed.shape[0]
    chunks = here.shape[2] // 128
    flip = edge[2] == 1

    def window(at):
        a, b = one[at], two[at]
        return jnp.concatenate([jnp.where(flip, b, a), here[at], jnp.where(flip, a, b)], axis=0)

    source = window(fields)
    for q in range(3):
        for i in range(chunks):
            scratch[q, i * 32 + 24 : i * 32 + 32, :] = jnp.zeros((8, 128), F32)

    def finest(fine, field, _):
        k = window(field)
        us, rs, rw, share = sweep(k, source, None, 0, 24, edge)
        parts[pl.ds(pl.multiple_of(field * 8, 8), 8), :] = summed(pieces(share[8:16]))
        if fine:
            rims[field, 0:1, :] = k[7:8]
            rims[field, 1:2, :] = k[16:17]
            rims[field, 2:3, :] = us[7:8]
            rims[field, 3:4, :] = us[16:17]
        for q, x in enumerate((k, rs, rw)):
            tall, rows = pairs_of_rows(x, scratch.at[q])
            for i in range(chunks):
                into = even if i % 2 == 0 else odd
                at = pl.multiple_of((q * (chunks // 2) + i // 2) * fields * rows + field * rows, 8)
                into[pl.ds(at, rows), :] = tall[i * rows : (i + 1) * rows]
        return 0

    lax.fori_loop(0, slots, functools.partial(finest, True), 0)
    lax.fori_loop(slots, fields, functools.partial(finest, False), 0)

    block = fields * 16
    level = []
    for q in range(3):
        span = slice(q * (chunks // 2) * block, (q + 1) * (chunks // 2) * block)
        got = dot(jnp.concatenate([even[span, :], odd[span, :]], axis=1), quarter)
        level.append(jnp.concatenate([got[i * block : (i + 1) * block] for i in range(chunks // 2)], axis=1))
    for depth, room in ((1, 16), (2, 8)):
        k, s, w = level
        us, rs, rw, share = sweep(k, s, w, depth, room, edge)
        own = 8 >> depth
        row = iota(share.shape, 0) % room
        share = summed(pieces(jnp.where((row >= own) & (row < 2 * own), share, 0.0))) * (16.0**depth)
        for field in range(fields):
            at = field * room
            parts[field * 8 : field * 8 + 8, :] += summed([share[at + i : at + i + 8] for i in range(0, room, 8)])
        kept = slots * room
        if depth == 1:
            s1_out[...], k1_out[...] = s[:kept], k[:kept]
        else:
            s2_out[...], k2_out[...] = s[:kept], k[:kept]
            to_far[...] = jnp.zeros_like(to_far)
            to_near[...] = jnp.zeros_like(to_near)
            for slot in range(slots):
                upper, lower = us[slot * 8 + 2 : slot * 8 + 3] * 16.0, us[slot * 8 + 3 : slot * 8 + 4] * 16.0
                to_far[slot : slot + 1, :] = jnp.where(flip, upper, lower)
                to_near[slot : slot + 1, :] = jnp.where(flip, lower, upper)
        level = [halve(x, scratch.at[q], quarter) for q, x in enumerate((k, rs, rw))]

    for q, x in enumerate(level):
        for field in range(fields):
            for h in range(2):
                line = x[field * 4 + 1 : field * 4 + 2, h * 128 : (h + 1) * 128]
                packed[0, (q * fields + field) * 2 + h : (q * fields + field) * 2 + h + 1, :] = line
    lane = iota((1, 128), 1)
    line = jnp.zeros((1, 128), F32)
    for field in range(fields):
        line = line + jnp.where(lane == field, jnp.sum(parts[field * 8 : field * 8 + 8, :]), 0.0)
    packed[0, 6 * fields : 6 * fields + 1, :] = line
    packed[0, 6 * fields + 1 :, :] = jnp.zeros((LINES - 6 * fields - 1, 128), F32)
    for i in range(1, copies):
        packed[i] = packed[0]


def shared_lines(fields):
    slots = fields // 2
    common = [(q * fields + f) * 2 + h for q in range(2) for f in range(slots) for h in range(2)]
    return common, lambda x: [(q * fields + slots + min(x, slots - 1)) * 2 + h for q in range(3) for h in range(2)]


def fan_kernel(lines, wide, *, fields):
    outer = wide.shape[0]
    common, special = shared_lines(fields)
    rows = wide.shape[1] // (len(common) + 6)
    for at, line in enumerate(common):
        got = lines[pl.ds(line, rows, stride=LINES), :]
        for x in range(outer):
            wide[x, at * rows : (at + 1) * rows, :] = got
    for x in range(outer):
        for at, line in enumerate(special(x)):
            start = (len(common) + at) * rows
            wide[x, start : start + rows, :] = lines[pl.ds(line, rows, stride=LINES), :]


def coarse_kernel(place, gathered, lines, e3, message, scratch, whole, *, fields, slabs, rows, cells):
    slots = fields // 2
    quarter = pair_matrix((256, 128), 0, 0.25)
    spread = pair_matrix((128, 256), 1, 1.0)
    n = slabs
    outer = gathered.shape[0]
    common = 4 * slots

    def taken(at):
        return jnp.concatenate([gathered[x, at * rows : (at + 1) * rows, :] for x in range(outer)], axis=0)

    def field(q, f):
        if f == slots:
            return jnp.concatenate([taken(common + q * 2), taken(common + q * 2 + 1)], axis=1)
        return jnp.concatenate([taken((q * slots + f) * 2), taken((q * slots + f) * 2 + 1)], axis=1)

    k3, s3 = [jnp.concatenate([field(q, f) for f in range(slots + 1)], axis=0) for q in range(2)]
    half3, fr3, fd3, diag3 = faces(k3, 256, n)
    scale3 = OMEGA / diag3
    u3 = scale3 * s3
    k4 = halve(k3, scratch.at[0], quarter)
    s4 = halve(s3 - fluxes(u3, half3, fr3, fd3, 256, n), scratch.at[1], quarter)
    half4, fr4, fd4, diag4 = faces(k4, 128, n // 2)
    scale4 = OMEGA / diag4
    u4 = scale4 * s4
    k5 = halve(k4, scratch.at[0], quarter)
    s5 = halve(s4 - fluxes(u4, half4, fr4, fd4, 128, n // 2), scratch.at[1], quarter)
    half5, fr5, fd5, diag5 = faces(k5, 64, n // 4)
    scale5 = jnp.where(iota(diag5.shape, 1) < 64, OMEGA / diag5, 0.0)
    u5 = scale5 * s5
    for _ in range(3):
        u5 = u5 + scale5 * (s5 - fluxes(u5, half5, fr5, fd5, 64, n // 4))
    u4 = u4 + double_rows(double_cols(u5, spread[:, :128]), scratch.at[0]) * 4.0
    u4 = u4 + scale4 * (s4 - fluxes(u4, half4, fr4, fd4, 128, n // 2))
    u3 = u3 + double_rows(double_cols(u4, spread), scratch.at[0]) * 4.0
    u3 = u3 + scale3 * (s3 - fluxes(u3, half3, fr3, fd3, 256, n))
    v3 = u3 * 64.0
    whole[0:8, :] = jnp.zeros((8, 256), F32)
    whole[8 : 8 + slots * n, :] = v3[: slots * n]
    whole[8 + slots * n :, :] = jnp.zeros((8, 256), F32)

    lane = iota((1, 128), 1)
    block = pl.multiple_of(place[5] * rows, 8)

    def weighed(f):
        v = whole[pl.ds(8 + f * n + block, rows), :]
        w = [lines[pl.ds((2 * fields + f) * 2 + h, rows, stride=LINES), :] for h in range(2)]
        return v[:, :128] * w[0] + v[:, 128:] * w[1]

    total = jnp.sum(lines[pl.ds(6 * fields, rows, stride=LINES), :], axis=0, keepdims=True)
    total = total - pltpu.roll(total, 128 - slots, 1)
    for f in range(slots):
        total = total + jnp.where(lane == f, 64.0 * jnp.sum(weighed(f)), 0.0)
    other = field(2, slots) * v3[slots * n :]
    total = total - jnp.where((lane == place[5]) & (lane < slots), 64.0 * jnp.sum(other), 0.0)
    sent = jnp.where(lane < slots, total / cells, jnp.where(lane == slots, place[7].astype(F32), 0.0))
    for i in range(message.shape[0]):
        message[i] = sent

    me = place[4]
    e3[...] = jnp.zeros_like(e3)
    for f in range(slots):
        for r in range(3):
            line = whole[pl.ds(8 + f * n + me + (r - 1), 1), :]
            if r == 0:
                line = jnp.where(me > 0, line, 0.0)
            if r == 2:
                line = jnp.where(me < n - 1, line, 0.0)
            e3[f * 8 + r : f * 8 + r + 1, :] = line


def up_kernel(edge, here, rims, s1, s2, k1, k2, e3, far, near, out, scratch):
    spread = pair_matrix((128, 256), 1, 1.0)
    slots = out.shape[0]

    def relaxed(k, s, e, depth, window, swap):
        half, fr, fd, diag = faces(k, k.shape[1], None)
        scale = OMEGA / diag
        s = s * (4.0**depth)
        valid = inside(k.shape, depth, edge, window)
        v = jnp.where(valid, swap(scale * s) + e, 0.0)
        return jnp.where(valid, v + scale * (s - fluxes(v, half, fr, fd, k.shape[1], None)), 0.0)

    def stacked(ref, rows):
        return jnp.concatenate([jnp.broadcast_to(ref[f : f + 1, :], (rows, ref.shape[1])) for f in range(slots)], axis=0)

    def rimmed(v):
        row = iota(v.shape, 0) % 8
        flip = edge[2] == 1
        a, b = stacked(far, 8), stacked(near, 8)
        return jnp.where(row == 0, jnp.where(flip, b, a), jnp.where(row == 5, jnp.where(flip, a, b), v))

    e = double_rows(double_cols(e3[...], spread), scratch)
    e = jnp.concatenate([e[f * 16 : f * 16 + 8] for f in range(slots)], axis=0)
    e = relaxed(k2[...], s2[...], e, 2, 8, rimmed)
    e = double_rows(double_cols(e, spread), scratch)
    e = relaxed(k1[...], s1[...], e, 1, 16, lambda v: v)
    e = double_cols(e, spread)
    g = here[2 * slots]
    row = iota(g.shape, 0)
    cols = g.shape[1]

    def lower(x, last):
        return jnp.where(row == 7, last, pltpu.roll(x, 7, 0))

    def upper(x, first):
        return jnp.where(row == 0, first, pltpu.roll(x, 1, 0))

    for f in range(slots):
        k = here[f]
        half = 0.5 * k
        fr = half + right_of(half, cols)
        fl = first_column(pltpu.roll(fr, 1, 1), half)
        fd = half + lower(half, 0.5 * rims[f, 1:2, :])
        fu = half + upper(half, 0.5 * rims[f, 0:1, :])
        scale = OMEGA / ((fr + fl) + (fd + fu))
        at = f * 16
        v = scale * g + double_rows(e[at : at + 8], scratch)[8:16]
        first = rims[f, 2:3, :] + e[at + 3 : at + 4]
        last = rims[f, 3:4, :] + e[at + 8 : at + 9]
        flow = across(v, half, fr, cols) + (fd * (v - lower(v, last)) + fu * (v - upper(v, first)))
        out[f] = v + scale * (g - flow)


def final_kernel(place, got, diffs, moments, estimate, *, levels, outer):
    slots = diffs.shape[0]
    row, lane = iota((8, 128), 0), iota((8, 128), 1)
    table = jnp.zeros((8, 128), F32)
    for m in range(levels):
        table = jnp.where(row == m, summed([got[m * outer + i] for i in range(outer)]), table)

    def along(x):
        return jnp.sum(x, axis=1, keepdims=True)

    counted = along(jnp.where(lane == slots, table, 0.0)) / outer
    counted = jnp.where(row[:, :1] < levels, counted, 1.0)
    live = (lane < slots) & (lane.astype(F32) < counted) & (row < levels)
    mean = along(jnp.where(live, table, 0.0)) / counted
    spare = jnp.where(live, table - mean, 0.0)
    var = along(spare * spare) / jnp.maximum(counted - 1.0, 1.0)
    both = jnp.where(lane == 0, mean, jnp.where(lane == 1, var, 0.0))
    sums = jnp.where(lane == 0, mean, jnp.where(lane == 1, var / counted, 0.0))
    sums = jnp.sum(sums, axis=0, keepdims=True)
    mine = row == place[6]
    own = jnp.sum(jnp.where(mine, table, 0.0), axis=0, keepdims=True)
    both = jnp.sum(jnp.where(mine, both, 0.0), axis=0, keepdims=True)
    for i in range(slots):
        diffs[i] = own[0, i]
    for i in range(2):
        moments[0, i] = both[0, i]
        estimate[i] = sums[0, i]


VMEM = pl.BlockSpec(memory_space=pltpu.VMEM)
SMEM = pl.BlockSpec(memory_space=pltpu.SMEM)


def shape(*dims):
    return jax.ShapeDtypeStruct(dims, F32)


def call(kernel, outs, smem, vmem, scratch, flops, mib, scalars=0):
    return pl.pallas_call(
        kernel,
        out_shape=outs,
        in_specs=[SMEM] * len(smem) + [VMEM] * len(vmem),
        out_specs=[VMEM] * (len(outs) - scalars) + [SMEM] * scalars,
        scratch_shapes=[pltpu.VMEM(s, F32) for s in scratch],
        compiler_params=pltpu.CompilerParams(vmem_limit_bytes=mib << 20),
        cost_estimate=pl.CostEstimate(flops=flops, bytes_accessed=1 << 20, transcendentals=0),
    )(*smem, *vmem)


def on_device(coef_fine, coef_coarse, rhs_field, level_counts):
    slots, rows, cols = coef_fine.shape
    fields = 2 * slots
    outer, inner = lax.axis_size("slab_0"), lax.axis_size("slab_1")
    levels = lax.axis_size("level")
    slabs = outer * inner
    me = lax.axis_index(SLAB)
    here = jnp.concatenate([coef_fine, coef_coarse, rhs_field[None]], axis=0)
    odd_down = [pair for i in range(1, slabs - 1, 2) for pair in ((i, i + 1), (i + 1, i))]
    odd_up = [pair for i in range(0, slabs, 2) for pair in ((i, i + 1), (i + 1, i))]
    one = lax.ppermute(here, SLAB, odd_down)
    two = lax.ppermute(here, SLAB, odd_up)
    x, z, level = [lax.axis_index(axis) for axis in ("slab_0", "slab_1", "level")]
    spot = [jnp.where(me == 0, 8, 0), jnp.where(me == slabs - 1, 16, 24), me % 2, z, me, x, level, level_counts[0]]
    edge = jnp.stack([jnp.asarray(value, jnp.int32) for value in spot])

    packed, rims, s1, s2, k1, k2, to_far, to_near = call(
        down_kernel,
        [
            shape(inner, LINES, 128),
            shape(slots, 8, cols),
            shape(slots * 16, cols // 2),
            shape(slots * 8, cols // 4),
            shape(slots * 16, cols // 2),
            shape(slots * 8, cols // 4),
            shape(8, cols // 4),
            shape(8, cols // 4),
        ],
        [edge],
        [here, one, two],
        [
            (3, max(cols // 4, 768), 128),
            (3 * fields * cols // 16, 128),
            (3 * fields * cols // 16, 128),
            (fields * 8, 128),
        ],
        20_000_000,
        28,
    )
    lines = lax.all_to_all(packed, "slab_1", 0, 0, tiled=True)
    far = lax.ppermute(to_far, SLAB, odd_down)
    near = lax.ppermute(to_near, SLAB, odd_up)
    lines, far, near = lax.optimization_barrier((lines, far, near))
    lines = lines.reshape(inner * LINES, 128)
    (wide,) = call(
        functools.partial(fan_kernel, fields=fields),
        [shape(outer, (4 * slots + 6) * inner, 128)],
        [],
        [lines],
        [],
        1_000_000,
        8,
    )
    gathered = lax.all_to_all(wide, "slab_0", 0, 0, tiled=True)
    e3, message = call(
        functools.partial(coarse_kernel, fields=fields, slabs=slabs, rows=inner, cells=float(rows * slabs * cols)),
        [shape(slots * 8, 256), shape(levels * outer, 1, 128)],
        [edge],
        [gathered, lines],
        [(2, 2 * (slots + 1) * slabs, 128), (slots * slabs + 16, 256)],
        5_000_000,
        16,
    )
    got = lax.all_to_all(message, ("level", "slab_0"), 0, 0, tiled=True)
    (solutions,) = call(
        up_kernel,
        [shape(slots, rows, cols)],
        [edge],
        [here, rims, s1, s2, k1, k2, e3, far, near],
        [(cols // 2, 128)],
        10_000_000,
        16,
    )
    diffs, moments, estimate = call(
        functools.partial(final_kernel, levels=levels, outer=outer),
        [shape(slots), shape(1, 2), shape(2)],
        [edge],
        [got],
        [],
        1_000,
        4,
        3,
    )
    return solutions, diffs, moments, estimate


def solution(mesh):
    slabs = mesh.shape["slab"]
    outer = 4 if slabs >= 64 else 2
    split = Mesh(mesh.devices.reshape(mesh.shape["level"], outer, slabs // outer), ("level", "slab_0", "slab_1"))
    in_specs = (P("level", SLAB, None), P("level", SLAB, None), P(SLAB, None), P("level"))
    out_specs = (P("level", SLAB, None), P("level"), P("level", None), P())
    return jax.shard_map(on_device, mesh=split, in_specs=in_specs, out_specs=out_specs, check_vma=False)
```
